32 devices in a mesh: dp: 8 (over z, x), mp: 4 (over y, core).
Axes of the slice: x: 2, y: 2, z: 4, core: 2. Of those that a mesh axis runs over, the one named last changes fastest.
Arguments:
- values: bfloat16 [8192, 96, 128], P('dp', 'mp'), may hold values from -0.29882812 to 0.29882812
- block_ids: int32 [8192, 96], P('dp', 'mp'), may hold values from 0 to 2047
- labels: int32 [8192], P('dp'), may hold values from 0 to 1
- weights: float32 [1048576], P(('dp', 'mp')), may hold values from -2.4 to 2.4
- history: float32 [2, 8, 1048576], P(None, None, ('dp', 'mp')), as said below
- steps: float32 [1], replicated, may hold values from 0.3 to 1
Outputs:
- final_weights: float32 [1048576], P(('dp', 'mp'))
- last_gradient: float32 [1048576], P(('dp', 'mp'))
The draws below stay inside these ranges and needn't reach their ends.
Inputs may be any that keep to these rules, and one draw needn't show every extreme that they name: `block_ids`: block ids are block numbers within the group of 2048 blocks of their mp shard. `history`: for every stored pair the inner product of its step and its gradient change is positive.
All inputs are finite; a program needn't handle non-finite values.
Results may differ from the reference program's by a relative error of at most 0.00039.
Values may be sent and summed in bfloat16 or wider, within the bound.
No kernel may reach another device: no remote copies, remote signals or barrier semaphores. Data moves between devices by JAX's collectives and lax.ppermute only.
A program may use at most 128 MiB of HBM per device.

```python
import math
import jax
import jax.numpy as jnp
from jax import lax

BLOCK = 128
BLK_DEV = 256
ROWS_DEV = 1024
ACTIVE = 24
HIST = 8
ITERS = 1
EXAMPLES = 8192
SHARD_BLOCKS = 2048
FEATURES = 1048576
N_DP = 8
N_MP = 4


def draw_history(key, part):
    keys = jax.random.split(jax.random.fold_in(key, 7), 2)
    ramp = 1.0 + 2.0 * jnp.arange(FEATURES, dtype=jnp.float32) / FEATURES
    base = jax.random.normal(keys[0], (HIST, FEATURES), jnp.float32)
    step_part = 0.3 * base * ramp[None, :]
    factor = jnp.exp(jax.random.uniform(keys[1], (HIST, FEATURES), jnp.float32, jnp.log(0.1), jnp.log(0.5)))
    change_part = factor * step_part
    return jnp.stack([step_part, change_part], axis=0)


def touch_ends(array, own_key, smallest, largest):
    index_at = [jax.random.randint(jax.random.fold_in(own_key, axis), (), 0, length) for axis, length in enumerate(array.shape)]
    longest = array.shape.index(max(array.shape))
    next_to = index_at[:longest] + [(index_at[longest] + 1) % array.shape[longest]] + index_at[longest + 1:]
    return array.at[tuple(index_at)].set(smallest).at[tuple(next_to)].set(largest)


def level_of(own_key, dims, shards, least, high):
    def one(position, blocks):
        steps = jax.random.uniform(jax.random.fold_in(jax.random.fold_in(own_key, 6), position), (blocks,), jnp.float32, least / len(shards), high / len(shards))
        return jnp.repeat(jnp.exp(steps), dims[position] // blocks).reshape((-1,) + (1,) * (len(dims) - position - 1))

    loudness = one(*shards[0])
    for cut in shards[1:]:
        loudness = loudness * one(*cut)
    return loudness


def centred(own_key, extent, width, reach, cuts=(), kind=jnp.bfloat16):
    drawn = width * jax.random.normal(own_key, extent, jnp.float32)
    if cuts:
        drawn = drawn * level_of(own_key, extent, cuts, -0.22, 0.18)
    return jnp.clip(drawn, -reach, reach).astype(kind)


def setup_inputs(seed: int = 0) -> dict:
    seeds = jax.random.split(jax.random.key(seed), 7)
    values = centred(seeds[0], (EXAMPLES, N_MP * ACTIVE, BLOCK), 0.05, 0.29882812, ((0, 8), (1, 4)))
    block_ids = touch_ends(jax.random.randint(seeds[1], (EXAMPLES, N_MP * ACTIVE), 0, SHARD_BLOCKS), jax.random.fold_in(seeds[1], 1), 0, SHARD_BLOCKS - 1).astype(jnp.int32)
    labels = touch_ends(jax.random.randint(seeds[2], (EXAMPLES,), 0, 2), jax.random.fold_in(seeds[2], 1), 0, 1).astype(jnp.int32)
    weights = centred(seeds[3], (FEATURES,), 0.4, 2.4, ((0, 32),), jnp.float32)
    history = draw_history(jax.random.fold_in(seeds[6], 71), 0)
    steps = jnp.clip(jnp.exp(jax.random.uniform(seeds[5], (ITERS,), jnp.float32, math.log(0.3), math.log(1.0))), 0.3, 1.0)
    return dict(values=values, block_ids=block_ids, labels=labels, weights=weights, history=history, steps=steps)


ridge = 0.2


def shard_view(vector):
    return vector.reshape(N_DP, N_MP, BLK_DEV, BLOCK).transpose(1, 0, 2, 3).reshape(N_MP, N_DP * BLK_DEV, BLOCK)


def flat_view(table):
    return table.reshape(N_MP, N_DP, BLK_DEV, BLOCK).transpose(1, 0, 2, 3).reshape(-1)


def gradient(current, values, block_ids, labels):
    table = shard_view(current).astype(jnp.bfloat16)
    vals = values.reshape(N_DP, ROWS_DEV, N_MP, ACTIVE, BLOCK)
    ids = block_ids.reshape(N_DP, ROWS_DEV, N_MP, ACTIVE).astype(jnp.int32)
    labs = labels.reshape(N_DP, ROWS_DEV)
    group = jnp.arange(N_MP, dtype=jnp.int32)[None, :, None]

    def step_rows(total, item):
        block_vals, block_idx, block_lab = item
        entries = block_vals.astype(jnp.float32)
        picked = table[group, block_idx].astype(jnp.float32)
        parts = jnp.sum(entries * picked, axis=(2, 3))
        margin = jnp.sum(parts, axis=1)
        resid = jax.nn.sigmoid(margin) - block_lab.astype(jnp.float32)
        contrib = entries * resid[:, None, None, None]
        index = (group * SHARD_BLOCKS + block_idx).reshape(-1).astype(jnp.int32)
        total = total + jax.ops.segment_sum(contrib.reshape(-1, BLOCK), index, num_segments=N_MP * SHARD_BLOCKS)
        return total, None

    start = jnp.zeros((N_MP * SHARD_BLOCKS, BLOCK), jnp.float32)
    total, _ = lax.scan(step_rows, start, (vals, ids, labs))
    return flat_view(total) + ridge * current


def direction(s_hist, y_hist, grad):
    count = s_hist.shape[0]
    rho = [1.0 / jnp.sum(s_hist[i] * y_hist[i]) for i in range(count)]
    alphas = [None] * count
    running = grad
    for i in reversed(range(count)):
        alphas[i] = rho[i] * jnp.sum(s_hist[i] * running)
        running = running - alphas[i] * y_hist[i]
    scale = jnp.sum(s_hist[-1] * y_hist[-1]) / jnp.sum(y_hist[-1] * y_hist[-1])
    running = scale * running
    for i in range(count):
        beta = rho[i] * jnp.sum(y_hist[i] * running)
        running = running + (alphas[i] - beta) * s_hist[i]
    return -running


def reference(values, block_ids, labels, weights, history, steps):
    s_hist = history[0]
    y_hist = history[1]
    current = weights
    grad = gradient(current, values, block_ids, labels)
    for k in range(ITERS):
        move = steps[k] * direction(s_hist, y_hist, grad)
        current = current + move
        if k + 1 < ITERS:
            new_grad = gradient(current, values, block_ids, labels)
            s_hist = jnp.concatenate([s_hist[1:], move[None]], axis=0)
            y_hist = jnp.concatenate([y_hist[1:], (new_grad - grad)[None]], axis=0)
            grad = new_grad
    return current, grad
```

```python
import functools

import jax
import jax.numpy as jnp
from jax import lax
from jax.experimental import pallas as pl
from jax.experimental.pallas import tpu as pltpu
from jax.sharding import PartitionSpec as P

ridge = 0.2
SUB = 8
F32 = jnp.float32


def sublane_masks():
    sub = lax.broadcasted_iota(jnp.int32, (SUB, 128), 0)
    return [sub == s for s in range(SUB)]


def vmem_spec():
    return pl.BlockSpec(memory_space=pltpu.VMEM)


def smem_spec():
    return pl.BlockSpec(memory_space=pltpu.SMEM)


def params(megabytes):
    return pltpu.CompilerParams(vmem_limit_bytes=int(megabytes * 2**20))


def mib(*arrays):
    return sum(a.size * a.dtype.itemsize for a in arrays) / 2**20


def gram_body(hist, out):
    count, feats = hist.shape[1], hist.shape[2]
    width = 128

    def step(j, accs):
        at = pl.ds(pl.multiple_of(j * width, width), width)
        s_tile, y_tile = hist[0, :, at], hist[1, :, at]
        new = []
        for i in range(count):
            row = jnp.broadcast_to(y_tile[i : i + 1, :], (count, width))
            new.append((accs[i][0] + row * s_tile, accs[i][1] + row * y_tile))
        return tuple(new)

    zero = jnp.zeros((count, width), F32)
    accs = lax.fori_loop(0, feats // width, step, tuple((zero, zero) for _ in range(count)))
    lane = lax.broadcasted_iota(jnp.int32, (count, width), 1)
    for part in range(2):
        tile = zero
        for i in range(count):
            tile = jnp.where(lane == i, jnp.sum(accs[i][part], axis=1, keepdims=True), tile)
        out[part * count : (part + 1) * count, :] = tile


def gather_body(ids, vals, gram, *refs):
    *pieces, out, table, rows = refs
    count, active, width = vals.shape
    at = 0
    for piece in pieces:
        size = piece.shape[0]

        def widen(j, carry, piece=piece, at=at):
            src = pl.ds(pl.multiple_of(j * 64, 64), 64)
            dst = pl.ds(pl.multiple_of(j * 64 + at, 64), 64)
            table[dst, :] = piece[src, :].astype(F32)
            return carry

        lax.fori_loop(0, size // 64, widen, 0)
        at += size
    masks = sublane_masks()

    def group(g, carry):
        tile = jnp.zeros((SUB, width), F32)
        for u in range(SUB):
            e = g * SUB + u
            v = vals[e].astype(F32)
            total = None
            for t in range(0, active, SUB):
                pick = None
                for s in range(SUB):
                    row = table[pl.ds(ids[(t + s) * count + e], SUB, stride=0), :]
                    pick = row if pick is None else jnp.where(masks[s], row, pick)
                prod = pick * v[t : t + SUB]
                total = prod if total is None else total + prod
            total = jnp.sum(total, axis=0, keepdims=True)
            tile = jnp.where(masks[u], jnp.broadcast_to(total, (SUB, width)), tile)
        rows[pl.ds(pl.multiple_of(g * SUB, SUB), SUB), :] = tile
        return carry

    lax.fori_loop(0, count // SUB, group, 0)
    lines = count // width
    for b in range(lines):
        flipped = rows[b * width : (b + 1) * width, :].T
        out[b : b + 1, :] = jnp.sum(flipped, axis=0, keepdims=True)
    out[lines : lines + gram.shape[0], :] = gram[...]


def scatter_body(ids, resid, vals, gram, *refs, order, owned):
    n_out = 2
    outs, accs = refs[:n_out], refs[n_out:]
    count, active, width = vals.shape
    blocks = accs[0].shape[0] // SUB
    masks = sublane_masks()
    zero = jnp.zeros((SUB * SUB, width), F32)

    def clear(j, carry):
        at = pl.ds(pl.multiple_of(j * SUB * SUB, SUB * SUB), SUB * SUB)
        for acc in accs:
            acc[at, :] = zero
        return carry

    lax.fori_loop(0, blocks // SUB, clear, 0)
    n_acc = len(accs)
    unroll = 4

    def example(e):
        r = resid[e]
        v = vals[e].astype(F32) * r
        tiles = list(range(0, active, SUB))
        for first in range(0, len(tiles), n_acc):
            batch = []
            for a, t in enumerate(tiles[first : first + n_acc]):
                part = v[t : t + SUB]
                for s in range(SUB):
                    at = pl.ds(pl.multiple_of(ids[(t + s) * count + e] * SUB, SUB), SUB)
                    batch.append((a, s, at, accs[a][at, :] + part))
            for a, s, at, value in batch:
                pltpu.store(accs[a].at[at, :], value, mask=masks[s])

    def group(g, carry):
        for u in range(unroll):
            example(g * unroll + u)
        return carry

    lax.fori_loop(0, count // unroll, group, 0)

    half = len(order) // 2
    for i, p in enumerate(order):
        out = outs[0] if i < half else outs[1]

        def fold(j, carry, p=p, out=out, base=(i % half) * owned):
            total = None
            at = pl.ds(pl.multiple_of((p * owned + j * SUB) * SUB, SUB * SUB), SUB * SUB)
            for acc in accs:
                x = acc[at, :].reshape(SUB, SUB, width)
                total = x if total is None else total + x
            out[pl.ds(pl.multiple_of(base + j * SUB, SUB), SUB), :] = jnp.sum(total, axis=1)
            return carry

        lax.fori_loop(0, owned // SUB, fold, 0)
    for out in outs:
        out[half * owned :, :] = gram[...]


def dots_body(keep, recv, w, hist, grad, dots, gram):
    count, feats = hist.shape[1], hist.shape[2]
    rows, width = w.shape
    grad[...] = keep[:rows, :] + recv[:rows, :] + ridge * w[...]
    gram[...] = keep[rows:, :] + recv[rows:, :]

    def step(j, accs):
        at = pl.ds(pl.multiple_of(j * width, width), width)
        g = grad[pl.ds(j, count, stride=0), :]
        return (accs[0] + g * hist[0, :, at], accs[1] + g * hist[1, :, at])

    zero = jnp.zeros((count, width), F32)
    accs = lax.fori_loop(0, feats // width, step, (zero, zero), unroll=8)
    dots[:count, :] = accs[0]
    dots[count:, :] = accs[1]


def coefficient_body(gram, out):
    count = gram.shape[0] // 2
    width = 128
    lane = lax.broadcasted_iota(jnp.int32, (1, width), 1)
    sy = lambda k, i: gram[k, i]
    yy = lambda k, i: gram[count + k, i]
    unit = lambda k: (lane == k).astype(F32)
    rho = [1.0 / jnp.full((1, width), sy(i, i), F32) for i in range(count)]
    last = count - 1
    gamma = jnp.full((1, width), sy(last, last), F32) / jnp.full((1, width), yy(last, last), F32)
    alpha = [None] * count
    for i in reversed(range(count)):
        value = unit(i)
        for j in range(i + 1, count):
            value = value - alpha[j] * sy(i, j)
        alpha[i] = rho[i] * value
    weight = []
    for i in range(count):
        value = unit(count + i)
        for j in range(count):
            value = value - alpha[j] * yy(i, j)
        value = gamma * value
        for k in range(i):
            value = value + weight[k] * sy(k, i)
        weight.append(alpha[i] - rho[i] * value)
    for k in range(count):
        out[k : k + 1, :] = weight[k]
        out[count + k : count + k + 1, :] = -gamma * alpha[k]
    out[2 * count :, :] = jnp.broadcast_to(gamma, (count, width))


def move_body(steps, coef, dots, recv, grad, w, hist, out):
    count = hist.shape[1]
    rows, width = w.shape
    sums = jnp.sum(dots[...] + recv[...], axis=1, keepdims=True)
    sub = lax.broadcasted_iota(jnp.int32, (2 * count, width), 0)
    lane = lax.broadcasted_iota(jnp.int32, (2 * count, width), 1)
    line = jnp.sum(jnp.where(sub == lane, sums, 0.0), axis=0, keepdims=True)
    mixed = jnp.sum(coef[: 2 * count, :] * line, axis=1, keepdims=True)
    c_s = jnp.broadcast_to(mixed[:count], (count, width))
    c_y = jnp.broadcast_to(mixed[count:], (count, width))
    gamma = coef[2 * count :, :]
    rate = steps[0]
    masks = sublane_masks()

    def step(j, carry):
        tile = jnp.zeros((SUB, width), F32)
        for u in range(SUB):
            at = pl.ds(pl.multiple_of((j * SUB + u) * width, width), width)
            mix = jnp.sum(c_s * hist[0, :, at] + c_y * hist[1, :, at], axis=0, keepdims=True)
            tile = jnp.where(masks[u], jnp.broadcast_to(mix, (SUB, width)), tile)
        at = pl.ds(pl.multiple_of(j * SUB, SUB), SUB)
        out[at, :] = w[at, :] - rate * (gamma * grad[at, :] + tile)
        return carry

    lax.fori_loop(0, rows // SUB, step, 0)


def gather_stages(n):
    stages = []
    top = n // 2
    while top >= 4:
        stages.append([top])
        top //= 2
    stages.append([k for k in (1, 2, 3) if k < n])
    return [s for s in stages if s]


def reduce_bits(n):
    bits = []
    b = 1
    while b < n:
        bits.append(b)
        b *= 2
    return bits


def xor_permute(x, axis, n, k):
    return lax.ppermute(x, axis, [(i, i ^ k) for i in range(n)])


def local(values, block_ids, labels, weights, history, steps, *, n_dp, n_mp):
    count, active, width = values.shape
    features = weights.shape[0]
    owned = features // width
    blocks = owned * n_dp
    pairs = history.shape[1]
    lines = count // width
    me = lax.axis_index("dp")
    w2 = weights.reshape(owned, width)

    pieces = [w2.astype(jnp.bfloat16)]
    order = [0]
    for offsets in gather_stages(n_dp):
        whole = pieces[0] if len(pieces) == 1 else jnp.concatenate(pieces, axis=0)
        came = [xor_permute(whole, "dp", n_dp, k) for k in offsets]
        pieces = pieces + came
        order = order + [p ^ k for k in offsets for p in order]
    place = [0] * n_dp
    for at, p in enumerate(order):
        place[p] = at
    ids_t = block_ids.T
    owner = ids_t // owned
    spot = owner ^ me
    where = jnp.zeros_like(spot)
    for p in range(n_dp):
        where = jnp.where(spot == p, place[p], where)
    flat_ids = (where * owned + (ids_t - owner * owned)).reshape(-1)

    gram = pl.pallas_call(
        gram_body,
        out_shape=jax.ShapeDtypeStruct((2 * pairs, width), F32),
        in_specs=[vmem_spec()],
        out_specs=vmem_spec(),
        compiler_params=params(2 * mib(history) + 2),
    )(history)

    table_mib = blocks * width * 4 / 2**20
    packed = pl.pallas_call(
        gather_body,
        out_shape=jax.ShapeDtypeStruct((lines + 2 * pairs, width), F32),
        in_specs=[smem_spec(), vmem_spec(), vmem_spec()] + [vmem_spec()] * len(pieces),
        out_specs=vmem_spec(),
        scratch_shapes=[pltpu.VMEM((blocks, width), F32), pltpu.VMEM((count, width), F32)],
        compiler_params=params(mib(values) + 2 * table_mib + 6),
    )(flat_ids, values, gram, *pieces)

    packed = jnp.sum(lax.all_gather(packed, "mp", axis=0), axis=0)
    resid = jax.nn.sigmoid(packed[:lines].reshape(-1)) - labels.astype(F32)
    gram_rows = packed[lines:]

    bits = reduce_bits(n_dp)
    wanted = [0]
    for b in reversed(bits):
        wanted = [p ^ b for p in wanted] + wanted
    slots = [place[p] for p in wanted]

    acc_mib = SUB * table_mib
    room = (60 * 1024) / 1024 - mib(values) - table_mib - 6
    n_acc = max(1, min(active // SUB, int(room // acc_mib)))
    half = n_dp // 2 * owned + 2 * pairs
    send, keep = pl.pallas_call(
        functools.partial(scatter_body, order=slots, owned=owned),
        out_shape=[jax.ShapeDtypeStruct((half, width), F32)] * 2,
        in_specs=[smem_spec(), smem_spec(), vmem_spec(), vmem_spec()],
        out_specs=[vmem_spec(), vmem_spec()],
        scratch_shapes=[pltpu.VMEM((blocks * SUB, width), F32)] * n_acc,
        compiler_params=params(mib(values) + table_mib + n_acc * acc_mib + 3),
    )(flat_ids, resid, values, gram_rows)

    size = n_dp // 2
    tail = 2 * pairs
    for b in bits:
        came = xor_permute(send, "dp", n_dp, b)
        if size == 1:
            break
        total = keep + came
        size //= 2
        cut = size * owned
        total_gram = total[2 * cut :]
        send = jnp.concatenate([total[:cut], total_gram], axis=0)
        keep = jnp.concatenate([total[cut : 2 * cut], total_gram], axis=0)

    grad, dots, gram_all = pl.pallas_call(
        dots_body,
        out_shape=[
            jax.ShapeDtypeStruct((owned, width), F32),
            jax.ShapeDtypeStruct((2 * pairs, width), F32),
            jax.ShapeDtypeStruct((2 * pairs, width), F32),
        ],
        in_specs=[vmem_spec()] * 4,
        out_specs=[vmem_spec()] * 3,
        compiler_params=params(2 * mib(history) + 4),
    )(keep, came, w2, history)

    coef = pl.pallas_call(
        coefficient_body,
        out_shape=jax.ShapeDtypeStruct((3 * pairs, width), F32),
        in_specs=[smem_spec()],
        out_specs=vmem_spec(),
        compiler_params=params(4),
    )(gram_all)

    hops = [("mp", n_mp, b) for b in reduce_bits(n_mp)] + [("dp", n_dp, b) for b in bits]
    for axis, n, b in hops[:-1]:
        dots = dots + xor_permute(dots, axis, n, b)
    axis, n, b = hops[-1]
    other = xor_permute(dots, axis, n, b)

    moved = pl.pallas_call(
        move_body,
        out_shape=jax.ShapeDtypeStruct((owned, width), F32),
        in_specs=[smem_spec()] + [vmem_spec()] * 6,
        out_specs=vmem_spec(),
        compiler_params=params(2 * mib(history) + 4),
    )(steps, coef, dots, other, grad, w2, history)
    return moved.reshape(-1), grad.reshape(-1)


def solution(mesh):
    placed = (
        P("dp", "mp", None),
        P("dp", "mp"),
        P("dp"),
        P(("dp", "mp")),
        P(None, None, ("dp", "mp")),
        P(),
    )
    return jax.shard_map(
        functools.partial(local, n_dp=mesh.shape["dp"], n_mp=mesh.shape["mp"]),
        mesh=mesh,
        in_specs=placed,
        out_specs=(P(("dp", "mp")), P(("dp", "mp"))),
        check_vma=False,
    )
```

```python
import functools

import jax
import jax.numpy as jnp
from jax import lax
from jax.experimental import pallas as pl
from jax.experimental.pallas import tpu as pltpu
from jax.sharding import PartitionSpec as P

ridge = 0.2
SUB = 8
F32 = jnp.float32


def sublane_masks():
    sub = lax.broadcasted_iota(jnp.int32, (SUB, 128), 0)
    return [sub == s for s in range(SUB)]


def vmem_spec():
    return pl.BlockSpec(memory_space=pltpu.VMEM)


def smem_spec():
    return pl.BlockSpec(memory_space=pltpu.SMEM)


def any_spec():
    return pl.BlockSpec(memory_space=pl.ANY)


def hbm_spec():
    return pl.BlockSpec(memory_space=pltpu.HBM)


def entry(ref, base, offset):
    return ref.at[pl.ds(base + offset, 1)][0]


def params(megabytes):
    return pltpu.CompilerParams(vmem_limit_bytes=int(megabytes * 2**20))


def mib(*arrays):
    return sum(a.size * a.dtype.itemsize for a in arrays) / 2**20


def gram_body(hist, out):
    count, feats = hist.shape[1], hist.shape[2]
    width = 128

    def step(j, accs):
        at = pl.ds(pl.multiple_of(j * width, width), width)
        s_tile, y_tile = hist[0, :, at], hist[1, :, at]
        new = []
        for i in range(count):
            row = jnp.broadcast_to(y_tile[i : i + 1, :], (count, width))
            new.append((accs[i][0] + row * s_tile, accs[i][1] + row * y_tile))
        return tuple(new)

    zero = jnp.zeros((count, width), F32)
    accs = lax.fori_loop(0, feats // width, step, tuple((zero, zero) for _ in range(count)))
    lane = lax.broadcasted_iota(jnp.int32, (count, width), 1)
    for part in range(2):
        tile = zero
        for i in range(count):
            tile = jnp.where(lane == i, jnp.sum(accs[i][part], axis=1, keepdims=True), tile)
        out[part * count : (part + 1) * count, :] = tile


def chunk_copies(src, dst, sems):
    n = sems.shape[0]
    size = src.shape[0] // n
    return [pltpu.make_async_copy(src.at[pl.ds(c * size, size)], dst.at[pl.ds(c * size, size)], sems.at[c]) for c in range(n)]


def gather_body(ids_in, vals_in, gram, *refs):
    *pieces, out, table, rows, vals, ids, vals_sems, ids_sems = refs
    count, active, width = vals.shape
    copies = chunk_copies(vals_in, vals, vals_sems)
    id_copies = chunk_copies(ids_in, ids, ids_sems)
    for i, c in zip(id_copies, copies):
        i.start()
        c.start()
    at = 0
    for piece in pieces:
        size = piece.shape[0]

        def widen(j, carry, piece=piece, at=at):
            src = pl.ds(pl.multiple_of(j * 64, 64), 64)
            dst = pl.ds(pl.multiple_of(j * 64 + at, 64), 64)
            table[dst, :] = piece[src, :].astype(F32)
            return carry

        lax.fori_loop(0, size // 64, widen, 0)
        at += size
    masks = sublane_masks()

    def group(g, carry):
        tile = jnp.zeros((SUB, width), F32)
        for u in range(SUB):
            e = g * SUB + u
            v = vals[e].astype(F32)
            total = None
            for t in range(0, active, SUB):
                pick = None
                for s in range(SUB):
                    row = table[pl.ds(entry(ids, e * active, t + s), SUB, stride=0), :]
                    pick = row if pick is None else jnp.where(masks[s], row, pick)
                prod = pick * v[t : t + SUB]
                total = prod if total is None else total + prod
            total = jnp.sum(total, axis=0, keepdims=True)
            tile = jnp.where(masks[u], jnp.broadcast_to(total, (SUB, width)), tile)
        rows[pl.ds(pl.multiple_of(g * SUB, SUB), SUB), :] = tile
        return carry

    per = count // SUB // len(copies)
    for i, (a, c) in enumerate(zip(id_copies, copies)):
        a.wait()
        c.wait()
        lax.fori_loop(i * per, (i + 1) * per, group, 0)
    lines = count // width
    for b in range(lines):
        flipped = rows[b * width : (b + 1) * width, :].T
        out[b : b + 1, :] = jnp.sum(flipped, axis=0, keepdims=True)
    out[lines : lines + gram.shape[0], :] = gram[...]


def scatter_body(ids_in, resid, vals_in, gram, *refs, order, owned):
    n_out = 2
    outs, accs = refs[:n_out], refs[n_out:-4]
    vals, ids, vals_sems, ids_sems = refs[-4:]
    count, active, width = vals.shape
    copies = chunk_copies(vals_in, vals, vals_sems)
    id_copies = chunk_copies(ids_in, ids, ids_sems)
    for i, c in zip(id_copies, copies):
        i.start()
        c.start()
    blocks = accs[0].shape[0] // SUB
    masks = sublane_masks()
    zero = jnp.zeros((SUB * SUB, width), F32)

    def clear(j, carry):
        at = pl.ds(pl.multiple_of(j * SUB * SUB, SUB * SUB), SUB * SUB)
        for acc in accs:
            acc[at, :] = zero
        return carry

    lax.fori_loop(0, blocks // SUB, clear, 0)
    n_acc = len(accs)
    unroll = 4

    def example(e):
        r = resid[e]
        v = vals[e].astype(F32) * r
        tiles = list(range(0, active, SUB))
        for first in range(0, len(tiles), n_acc):
            batch = []
            for a, t in enumerate(tiles[first : first + n_acc]):
                part = v[t : t + SUB]
                for s in range(SUB):
                    at = pl.ds(pl.multiple_of(entry(ids, e * active, t + s), SUB), SUB)
                    batch.append((a, s, at, accs[a][at, :] + part))
            for a, s, at, value in batch:
                pltpu.store(accs[a].at[at, :], value, mask=masks[s])

    def group(g, carry):
        for u in range(unroll):
            example(g * unroll + u)
        return carry

    per = count // unroll // len(copies)
    for i, (a, c) in enumerate(zip(id_copies, copies)):
        a.wait()
        c.wait()
        lax.fori_loop(i * per, (i + 1) * per, group, 0)

    half = len(order) // 2
    for i, p in enumerate(order):
        out = outs[0] if i < half else outs[1]

        def fold(j, carry, p=p, out=out, base=(i % half) * owned):
            total = None
            at = pl.ds(pl.multiple_of((p * owned + j * SUB) * SUB, SUB * SUB), SUB * SUB)
            for acc in accs:
                x = acc[at, :].reshape(SUB, SUB, width)
                total = x if total is None else total + x
            out[pl.ds(pl.multiple_of(base + j * SUB, SUB), SUB), :] = jnp.sum(total, axis=1)
            return carry

        lax.fori_loop(0, owned // SUB, fold, 0, unroll=2)
    for out in outs:
        out[half * owned :, :] = gram[...]


def dots_body(keep, recv, w, hist, result, grad, dots, gram):
    count, feats = hist.shape[1], hist.shape[2]
    rows, width = w.shape
    grad[...] = keep[:rows, :] + recv[:rows, :] + ridge * w[...]
    result[...] = grad[...]
    gram[...] = keep[rows:, :] + recv[rows:, :]

    def step(j, accs):
        at = pl.ds(pl.multiple_of(j * width, width), width)
        g = grad[pl.ds(j, count, stride=0), :]
        return (accs[0] + g * hist[0, :, at], accs[1] + g * hist[1, :, at])

    zero = jnp.zeros((count, width), F32)
    accs = lax.fori_loop(0, feats // width, step, (zero, zero), unroll=8)
    dots[:count, :] = accs[0]
    dots[count:, :] = accs[1]


def coefficient_body(gram, out):
    count = gram.shape[0] // 2
    width = 128
    lane = lax.broadcasted_iota(jnp.int32, (1, width), 1)
    sy = lambda k, i: gram[k, i]
    yy = lambda k, i: gram[count + k, i]
    unit = lambda k: (lane == k).astype(F32)
    rho = [1.0 / jnp.full((1, width), sy(i, i), F32) for i in range(count)]
    last = count - 1
    gamma = jnp.full((1, width), sy(last, last), F32) / jnp.full((1, width), yy(last, last), F32)
    alpha = [None] * count
    for i in reversed(range(count)):
        value = unit(i)
        for j in range(i + 1, count):
            value = value - alpha[j] * sy(i, j)
        alpha[i] = rho[i] * value
    weight = []
    for i in range(count):
        value = unit(count + i)
        for j in range(count):
            value = value - alpha[j] * yy(i, j)
        value = gamma * value
        for k in range(i):
            value = value + weight[k] * sy(k, i)
        weight.append(alpha[i] - rho[i] * value)
    for k in range(count):
        out[k : k + 1, :] = weight[k]
        out[count + k : count + k + 1, :] = -gamma * alpha[k]
    out[2 * count :, :] = jnp.broadcast_to(gamma, (count, width))


def move_body(steps, coef, dots, recv, grad, w, hist, out):
    count = hist.shape[1]
    rows, width = w.shape
    sums = jnp.sum(dots[...] + recv[...], axis=1, keepdims=True)
    sub = lax.broadcasted_iota(jnp.int32, (2 * count, width), 0)
    lane = lax.broadcasted_iota(jnp.int32, (2 * count, width), 1)
    line = jnp.sum(jnp.where(sub == lane, sums, 0.0), axis=0, keepdims=True)
    mixed = jnp.sum(coef[: 2 * count, :] * line, axis=1, keepdims=True)
    c_s = jnp.broadcast_to(mixed[:count], (count, width))
    c_y = jnp.broadcast_to(mixed[count:], (count, width))
    gamma = coef[2 * count :, :]
    rate = steps[0]
    masks = sublane_masks()

    def step(j, carry):
        tile = jnp.zeros((SUB, width), F32)
        for u in range(SUB):
            at = pl.ds(pl.multiple_of((j * SUB + u) * width, width), width)
            mix = jnp.sum(c_s * hist[0, :, at] + c_y * hist[1, :, at], axis=0, keepdims=True)
            tile = jnp.where(masks[u], jnp.broadcast_to(mix, (SUB, width)), tile)
        at = pl.ds(pl.multiple_of(j * SUB, SUB), SUB)
        out[at, :] = w[at, :] - rate * (gamma * grad[at, :] + tile)
        return carry

    lax.fori_loop(0, rows // SUB, step, 0)


def gather_stages(n):
    stages = []
    top = n // 2
    while top >= 4:
        stages.append([top])
        top //= 2
    stages.append([k for k in (1, 2, 3) if k < n])
    return [s for s in stages if s]


def reduce_bits(n):
    bits = []
    b = 1
    while b < n:
        bits.append(b)
        b *= 2
    return bits


def xor_permute(x, axis, n, k):
    return lax.ppermute(x, axis, [(i, i ^ k) for i in range(n)])


def local(values, block_ids, labels, weights, history, steps, *, n_dp, n_mp):
    count, active, width = values.shape
    features = weights.shape[0]
    owned = features // width
    blocks = owned * n_dp
    pairs = history.shape[1]
    lines = count // width
    me = lax.axis_index("dp")
    w2 = weights.reshape(owned, width)
    values = pltpu.with_memory_space_constraint(values, pltpu.HBM)

    pieces = [w2.astype(jnp.bfloat16)]
    order = [0]
    for offsets in gather_stages(n_dp):
        whole = pieces[0] if len(pieces) == 1 else jnp.concatenate(pieces, axis=0)
        came = [xor_permute(whole, "dp", n_dp, k) for k in offsets]
        pieces = pieces + came
        order = order + [p ^ k for k in offsets for p in order]
    place = [0] * n_dp
    for at, p in enumerate(order):
        place[p] = at
    owner = block_ids // owned
    spot = owner ^ me
    where = jnp.zeros_like(spot)
    for p in range(n_dp):
        where = jnp.where(spot == p, place[p], where)
    flat_ids = (where * owned + (block_ids - owner * owned)).reshape(-1)

    gram = pl.pallas_call(
        gram_body,
        out_shape=jax.ShapeDtypeStruct((2 * pairs, width), F32),
        in_specs=[vmem_spec()],
        out_specs=vmem_spec(),
        compiler_params=params(2 * mib(history) + 2),
    )(history)

    streams = [
        pltpu.VMEM(values.shape, values.dtype),
        pltpu.SMEM((count * active,), jnp.int32),
        pltpu.SemaphoreType.DMA((8,)),
        pltpu.SemaphoreType.DMA((8,)),
    ]
    table_mib = blocks * width * 4 / 2**20
    packed = pl.pallas_call(
        gather_body,
        out_shape=jax.ShapeDtypeStruct((lines + 2 * pairs, width), F32),
        in_specs=[any_spec(), hbm_spec(), vmem_spec()] + [vmem_spec()] * len(pieces),
        out_specs=vmem_spec(),
        scratch_shapes=[pltpu.VMEM((blocks, width), F32), pltpu.VMEM((count, width), F32)] + streams,
        compiler_params=params(mib(values) + 2 * table_mib + 6),
    )(flat_ids, values, gram, *pieces)

    packed = jnp.sum(lax.all_gather(packed, "mp", axis=0), axis=0)
    resid = jax.nn.sigmoid(packed[:lines].reshape(-1)) - labels.astype(F32)
    gram_rows = packed[lines:]

    bits = reduce_bits(n_dp)
    wanted = [0]
    for b in reversed(bits):
        wanted = [p ^ b for p in wanted] + wanted
    slots = [place[p] for p in wanted]

    acc_mib = SUB * table_mib
    room = (60 * 1024) / 1024 - mib(values) - table_mib - 6
    n_acc = max(1, min(active // SUB, int(room // acc_mib)))
    half = n_dp // 2 * owned + 2 * pairs
    send, keep = pl.pallas_call(
        functools.partial(scatter_body, order=slots, owned=owned),
        out_shape=[jax.ShapeDtypeStruct((half, width), F32)] * 2,
        in_specs=[any_spec(), smem_spec(), hbm_spec(), vmem_spec()],
        out_specs=[vmem_spec(), vmem_spec()],
        scratch_shapes=[pltpu.VMEM((blocks * SUB, width), F32)] * n_acc + streams,
        compiler_params=params(mib(values) + table_mib + n_acc * acc_mib + 3),
    )(flat_ids * SUB, resid, values, gram_rows)

    size = n_dp // 2
    tail = 2 * pairs
    for b in bits:
        came = xor_permute(send, "dp", n_dp, b)
        if size == 1:
            break
        total = keep + came
        size //= 2
        cut = size * owned
        total_gram = total[2 * cut :]
        send = jnp.concatenate([total[:cut], total_gram], axis=0)
        keep = jnp.concatenate([total[cut : 2 * cut], total_gram], axis=0)

    result, grad, dots, gram_all = pl.pallas_call(
        dots_body,
        out_shape=[
            jax.ShapeDtypeStruct((owned, width), F32),
            jax.ShapeDtypeStruct((owned, width), F32),
            jax.ShapeDtypeStruct((2 * pairs, width), F32),
            jax.ShapeDtypeStruct((2 * pairs, width), F32),
        ],
        in_specs=[vmem_spec()] * 4,
        out_specs=[vmem_spec()] * 4,
        compiler_params=params(2 * mib(history) + 4),
    )(keep, came, w2, history)

    coef = pl.pallas_call(
        coefficient_body,
        out_shape=jax.ShapeDtypeStruct((3 * pairs, width), F32),
        in_specs=[smem_spec()],
        out_specs=vmem_spec(),
        compiler_params=params(4),
    )(gram_all)

    hops = [("mp", n_mp, b) for b in reduce_bits(n_mp)] + [("dp", n_dp, b) for b in bits]
    for axis, n, b in hops[:-1]:
        dots = dots + xor_permute(dots, axis, n, b)
    axis, n, b = hops[-1]
    other = xor_permute(dots, axis, n, b)

    moved = pl.pallas_call(
        move_body,
        out_shape=jax.ShapeDtypeStruct((owned, width), F32),
        in_specs=[smem_spec()] + [vmem_spec()] * 6,
        out_specs=vmem_spec(),
        compiler_params=params(2 * mib(history) + 4),
    )(steps, coef, dots, other, grad, w2, history)
    return moved.reshape(-1), result.reshape(-1)


def solution(mesh):
    placed = (
        P("dp", "mp", None),
        P("dp", "mp"),
        P("dp"),
        P(("dp", "mp")),
        P(None, None, ("dp", "mp")),
        P(),
    )
    return jax.shard_map(
        functools.partial(local, n_dp=mesh.shape["dp"], n_mp=mesh.shape["mp"]),
        mesh=mesh,
        in_specs=placed,
        out_specs=(P(("dp", "mp")), P(("dp", "mp"))),
        check_vma=False,
    )
```

```python
import functools

import jax
import jax.numpy as jnp
from jax import lax
from jax.experimental import pallas as pl
from jax.experimental.pallas import tpu as pltpu
from jax.sharding import PartitionSpec as P

ridge = 0.2
SUB = 8
MAX_ACC = 3
F32 = jnp.float32


def sublane_masks():
    sub = lax.broadcasted_iota(jnp.int32, (SUB, 128), 0)
    return [sub == s for s in range(SUB)]


def vmem_spec():
    return pl.BlockSpec(memory_space=pltpu.VMEM)


def smem_spec():
    return pl.BlockSpec(memory_space=pltpu.SMEM)


def any_spec():
    return pl.BlockSpec(memory_space=pl.ANY)


def hbm_spec():
    return pl.BlockSpec(memory_space=pltpu.HBM)


def entry(ref, base, offset):
    return ref.at[pl.ds(base + offset, 1)][0]


def params(megabytes):
    return pltpu.CompilerParams(vmem_limit_bytes=int(megabytes * 2**20))


def mib(*arrays):
    return sum(a.size * a.dtype.itemsize for a in arrays) / 2**20


def gram_body(hist, out):
    count, feats = hist.shape[1], hist.shape[2]
    width = 128

    def step(j, accs):
        at = pl.ds(pl.multiple_of(j * width, width), width)
        s_tile, y_tile = hist[0, :, at], hist[1, :, at]
        new = []
        for i in range(count):
            row = jnp.broadcast_to(y_tile[i : i + 1, :], (count, width))
            new.append((accs[i][0] + row * s_tile, accs[i][1] + row * y_tile))
        return tuple(new)

    zero = jnp.zeros((count, width), F32)
    accs = lax.fori_loop(0, feats // width, step, tuple((zero, zero) for _ in range(count)))
    lane = lax.broadcasted_iota(jnp.int32, (count, width), 1)
    for part in range(2):
        tile = zero
        for i in range(count):
            tile = jnp.where(lane == i, jnp.sum(accs[i][part], axis=1, keepdims=True), tile)
        out[part * count : (part + 1) * count, :] = tile


def chunk_copies(srcs, dsts, sems, c):
    n = sems.shape[1]
    copies = []
    for i, (src, dst) in enumerate(zip(srcs, dsts)):
        size = src.shape[0] // n
        at = pl.ds(c * size, size)
        copies.append(pltpu.make_async_copy(src.at[at], dst.at[at], sems.at[i, c]))
    return copies


def start_chunks(srcs, dsts, sems):
    for c in range(sems.shape[1]):
        for copy in chunk_copies(srcs, dsts, sems, c):
            copy.start()


def run_chunks(srcs, dsts, sems, trips, body):
    per = trips // sems.shape[1]

    def chunk(c, carry):
        for copy in chunk_copies(srcs, dsts, sems, c):
            copy.wait()
        return lax.fori_loop(c * per, (c + 1) * per, body, carry)

    lax.fori_loop(0, sems.shape[1], chunk, 0)


def fold_tiles(tiles):
    sub = lax.broadcasted_iota(jnp.int32, tiles[0].shape, 0)
    half = SUB // 2
    low = (sub & half) == 0
    tiles = [
        jnp.where(low, tiles[k], tiles[k + half]) + pltpu.roll(jnp.where(low, tiles[k + half], tiles[k]), half, 0)
        for k in range(half)
    ]
    while half > 1:
        half //= 2
        odd = (sub & half) != 0
        tiles = [
            jnp.where(
                odd,
                tiles[k + half] + pltpu.roll(tiles[k + half], half, 0),
                tiles[k] + pltpu.roll(tiles[k], SUB - half, 0),
            )
            for k in range(half)
        ]
    return tiles[0]


def gather_body(ids_in, vals_in, gram, *refs):
    *pieces, out, table, rows, vals, ids, sems = refs
    srcs, dsts = (ids_in, vals_in), (ids, vals)
    count, active, width = vals.shape
    start_chunks(srcs, dsts, sems)
    at = 0
    for piece in pieces:
        size = piece.shape[0]

        def widen(j, carry, piece=piece, at=at):
            src = pl.ds(pl.multiple_of(j * 64, 64), 64)
            dst = pl.ds(pl.multiple_of(j * 64 + at, 64), 64)
            table[dst, :] = piece[src, :].astype(F32)
            return carry

        lax.fori_loop(0, size // 64, widen, 0)
        at += size
    masks = sublane_masks()

    def group(g, carry):
        for u in range(SUB):
            e = g * SUB + u
            v = vals[e].astype(F32)
            total = None
            for t in range(0, active, SUB):
                pick = None
                for s in range(SUB):
                    row = table[pl.ds(entry(ids, e * active, t + s), SUB, stride=0), :]
                    pick = row if pick is None else jnp.where(masks[s], row, pick)
                prod = pick * v[t : t + SUB]
                total = prod if total is None else total + prod
            rows[pl.ds(e, 1), :] = jnp.sum(total, axis=0, keepdims=True)
        return carry

    run_chunks(srcs, dsts, sems, count // SUB, group)
    lines = count // width
    for b in range(lines):
        flipped = rows[b * width : (b + 1) * width, :].T
        out[b : b + 1, :] = jnp.sum(flipped, axis=0, keepdims=True)
    out[lines : lines + gram.shape[0], :] = gram[...]


def scatter_body(ids_in, resid, vals_in, gram, *refs, order, owned):
    n_out = 2
    outs, accs = refs[:n_out], refs[n_out:-3]
    vals, ids, sems = refs[-3:]
    srcs, dsts = (ids_in, vals_in), (ids, vals)
    count, active, width = vals.shape
    start_chunks(srcs, dsts, sems)
    blocks = accs[0].shape[0] // SUB
    masks = sublane_masks()
    zero = jnp.zeros((SUB * SUB, width), F32)

    def clear(j, carry):
        at = pl.ds(pl.multiple_of(j * SUB * SUB, SUB * SUB), SUB * SUB)
        for acc in accs:
            acc[at, :] = zero
        return carry

    lax.fori_loop(0, blocks // SUB, clear, 0)
    unroll = 8

    def group(g, carry):
        turn = 0
        for u in range(unroll):
            e = g * unroll + u
            v = vals[e].astype(F32) * resid[e]
            for t in range(0, active, SUB):
                acc = accs[turn % len(accs)]
                turn += 1
                batch = []
                for s in range(SUB):
                    at = pl.ds(pl.multiple_of(entry(ids, e * active, t + s), SUB), SUB)
                    batch.append((at, acc[at, :] + v[t : t + SUB]))
                for s, (at, value) in enumerate(batch):
                    pltpu.store(acc.at[at, :], value, mask=masks[s])
        return carry

    run_chunks(srcs, dsts, sems, count // unroll, group)

    half = len(order) // 2
    for i, p in enumerate(order):
        out = outs[0] if i < half else outs[1]

        def fold(j, carry, p=p, out=out, base=(i % half) * owned):
            tiles = []
            for i in range(SUB):
                at = pl.ds(pl.multiple_of((p * owned + j * SUB + i) * SUB, SUB), SUB)
                total = accs[0][at, :]
                for acc in accs[1:]:
                    total = total + acc[at, :]
                tiles.append(total)
            out[pl.ds(pl.multiple_of(base + j * SUB, SUB), SUB), :] = fold_tiles(tiles)
            return carry

        lax.fori_loop(0, owned // SUB, fold, 0, unroll=2)
    for out in outs:
        out[half * owned :, :] = gram[...]


def dots_body(keep, recv, w, hist, result, grad, dots, gram):
    count, feats = hist.shape[1], hist.shape[2]
    rows, width = w.shape
    grad[...] = keep[:rows, :] + recv[:rows, :] + ridge * w[...]
    result[...] = grad[...]
    gram[...] = keep[rows:, :] + recv[rows:, :]

    def step(j, accs):
        at = pl.ds(pl.multiple_of(j * width, width), width)
        g = grad[pl.ds(j, count, stride=0), :]
        return (accs[0] + g * hist[0, :, at], accs[1] + g * hist[1, :, at])

    zero = jnp.zeros((count, width), F32)
    accs = lax.fori_loop(0, feats // width, step, (zero, zero), unroll=8)
    dots[:count, :] = accs[0]
    dots[count:, :] = accs[1]


def coefficient_body(gram, out):
    count = gram.shape[0] // 2
    width = 128
    lane = lax.broadcasted_iota(jnp.int32, (1, width), 1)
    sy = lambda k, i: gram[k, i]
    yy = lambda k, i: gram[count + k, i]
    unit = lambda k: (lane == k).astype(F32)
    rho = [1.0 / jnp.full((1, width), sy(i, i), F32) for i in range(count)]
    last = count - 1
    gamma = jnp.full((1, width), sy(last, last), F32) / jnp.full((1, width), yy(last, last), F32)
    alpha = [None] * count
    for i in reversed(range(count)):
        value = unit(i)
        for j in range(i + 1, count):
            value = value - alpha[j] * sy(i, j)
        alpha[i] = rho[i] * value
    weight = []
    for i in range(count):
        value = unit(count + i)
        for j in range(count):
            value = value - alpha[j] * yy(i, j)
        value = gamma * value
        for k in range(i):
            value = value + weight[k] * sy(k, i)
        weight.append(alpha[i] - rho[i] * value)
    for k in range(count):
        out[k : k + 1, :] = weight[k]
        out[count + k : count + k + 1, :] = -gamma * alpha[k]
    out[2 * count :, :] = jnp.broadcast_to(gamma, (count, width))


def move_body(steps, coef, dots, recv, grad, w, hist, out):
    count = hist.shape[1]
    rows, width = w.shape
    sums = jnp.sum(dots[...] + recv[...], axis=1, keepdims=True)
    sub = lax.broadcasted_iota(jnp.int32, (2 * count, width), 0)
    lane = lax.broadcasted_iota(jnp.int32, (2 * count, width), 1)
    line = jnp.sum(jnp.where(sub == lane, sums, 0.0), axis=0, keepdims=True)
    mixed = jnp.sum(coef[: 2 * count, :] * line, axis=1, keepdims=True)
    c_s = jnp.broadcast_to(mixed[:count], (count, width))
    c_y = jnp.broadcast_to(mixed[count:], (count, width))
    gamma = coef[2 * count :, :]
    rate = steps[0]
    masks = sublane_masks()

    def step(j, carry):
        tile = jnp.zeros((SUB, width), F32)
        for u in range(SUB):
            at = pl.ds(pl.multiple_of((j * SUB + u) * width, width), width)
            mix = jnp.sum(c_s * hist[0, :, at] + c_y * hist[1, :, at], axis=0, keepdims=True)
            tile = jnp.where(masks[u], jnp.broadcast_to(mix, (SUB, width)), tile)
        at = pl.ds(pl.multiple_of(j * SUB, SUB), SUB)
        out[at, :] = w[at, :] - rate * (gamma * grad[at, :] + tile)
        return carry

    lax.fori_loop(0, rows // SUB, step, 0)


def gather_stages(n):
    stages = []
    top = n // 2
    while top >= 4:
        stages.append([top])
        top //= 2
    stages.append([k for k in (1, 2, 3) if k < n])
    return [s for s in stages if s]


def reduce_bits(n):
    bits = []
    b = 1
    while b < n:
        bits.append(b)
        b *= 2
    return bits


def xor_permute(x, axis, n, k):
    return lax.ppermute(x, axis, [(i, i ^ k) for i in range(n)])


def local(values, block_ids, labels, weights, history, steps, *, n_dp, n_mp):
    count, active, width = values.shape
    features = weights.shape[0]
    owned = features // width
    blocks = owned * n_dp
    pairs = history.shape[1]
    lines = count // width
    me = lax.axis_index("dp")
    w2 = weights.reshape(owned, width)
    values = pltpu.with_memory_space_constraint(values, pltpu.HBM)

    pieces = [w2.astype(jnp.bfloat16)]
    order = [0]
    for offsets in gather_stages(n_dp):
        whole = pieces[0] if len(pieces) == 1 else jnp.concatenate(pieces, axis=0)
        came = [xor_permute(whole, "dp", n_dp, k) for k in offsets]
        pieces = pieces + came
        order = order + [p ^ k for k in offsets for p in order]
    place = [0] * n_dp
    for at, p in enumerate(order):
        place[p] = at
    owner = block_ids // owned
    spot = owner ^ me
    where = jnp.zeros_like(spot)
    for p in range(n_dp):
        where = jnp.where(spot == p, place[p], where)
    flat_ids = (where * owned + (block_ids - owner * owned)).reshape(-1)

    gram = pl.pallas_call(
        gram_body,
        out_shape=jax.ShapeDtypeStruct((2 * pairs, width), F32),
        in_specs=[vmem_spec()],
        out_specs=vmem_spec(),
        compiler_params=params(2 * mib(history) + 2),
    )(history)

    streams = [
        pltpu.VMEM(values.shape, values.dtype),
        pltpu.SMEM((count * active,), jnp.int32),
        pltpu.SemaphoreType.DMA((2, 8)),
    ]
    table_mib = blocks * width * 4 / 2**20
    packed = pl.pallas_call(
        gather_body,
        out_shape=jax.ShapeDtypeStruct((lines + 2 * pairs, width), F32),
        in_specs=[any_spec(), hbm_spec(), vmem_spec()] + [vmem_spec()] * len(pieces),
        out_specs=vmem_spec(),
        scratch_shapes=[pltpu.VMEM((blocks, width), F32), pltpu.VMEM((count, width), F32)] + streams,
        compiler_params=params(mib(values) + 2 * table_mib + 6),
    )(flat_ids, values, gram, *pieces)

    packed = jnp.sum(lax.all_gather(packed, "mp", axis=0), axis=0)
    resid = jax.nn.sigmoid(packed[:lines].reshape(-1)) - labels.astype(F32)
    gram_rows = packed[lines:]

    bits = reduce_bits(n_dp)
    wanted = [0]
    for b in reversed(bits):
        wanted = [p ^ b for p in wanted] + wanted
    slots = [place[p] for p in wanted]

    acc_mib = SUB * table_mib
    room = (60 * 1024) / 1024 - mib(values) - table_mib - 6
    n_acc = max(1, min(MAX_ACC, int(room // acc_mib)))
    half = n_dp // 2 * owned + 2 * pairs
    send, keep = pl.pallas_call(
        functools.partial(scatter_body, order=slots, owned=owned),
        out_shape=[jax.ShapeDtypeStruct((half, width), F32)] * 2,
        in_specs=[any_spec(), smem_spec(), hbm_spec(), vmem_spec()],
        out_specs=[vmem_spec(), vmem_spec()],
        scratch_shapes=[pltpu.VMEM((blocks * SUB, width), F32)] * n_acc + streams,
        compiler_params=params(mib(values) + table_mib + n_acc * acc_mib + 3),
    )(flat_ids * SUB, resid, values, gram_rows)

    size = n_dp // 2
    tail = 2 * pairs
    for b in bits:
        came = xor_permute(send, "dp", n_dp, b)
        if size == 1:
            break
        total = keep + came
        size //= 2
        cut = size * owned
        total_gram = total[2 * cut :]
        send = jnp.concatenate([total[:cut], total_gram], axis=0)
        keep = jnp.concatenate([total[cut : 2 * cut], total_gram], axis=0)

    result, grad, dots, gram_all = pl.pallas_call(
        dots_body,
        out_shape=[
            jax.ShapeDtypeStruct((owned, width), F32),
            jax.ShapeDtypeStruct((owned, width), F32),
            jax.ShapeDtypeStruct((2 * pairs, width), F32),
            jax.ShapeDtypeStruct((2 * pairs, width), F32),
        ],
        in_specs=[vmem_spec()] * 4,
        out_specs=[vmem_spec()] * 4,
        compiler_params=params(2 * mib(history) + 4),
    )(keep, came, w2, history)

    coef = pl.pallas_call(
        coefficient_body,
        out_shape=jax.ShapeDtypeStruct((3 * pairs, width), F32),
        in_specs=[smem_spec()],
        out_specs=vmem_spec(),
        compiler_params=params(4),
    )(gram_all)

    hops = [("mp", n_mp, b) for b in reduce_bits(n_mp)] + [("dp", n_dp, b) for b in bits]
    for axis, n, b in hops[:-1]:
        dots = dots + xor_permute(dots, axis, n, b)
    axis, n, b = hops[-1]
    other = xor_permute(dots, axis, n, b)

    moved = pl.pallas_call(
        move_body,
        out_shape=jax.ShapeDtypeStruct((owned, width), F32),
        in_specs=[smem_spec()] + [vmem_spec()] * 6,
        out_specs=vmem_spec(),
        compiler_params=params(2 * mib(history) + 4),
    )(steps, coef, dots, other, grad, w2, history)
    return moved.reshape(-1), result.reshape(-1)


def solution(mesh):
    placed = (
        P("dp", "mp", None),
        P("dp", "mp"),
        P("dp"),
        P(("dp", "mp")),
        P(None, None, ("dp", "mp")),
        P(),
    )
    return jax.shard_map(
        functools.partial(local, n_dp=mesh.shape["dp"], n_mp=mesh.shape["mp"]),
        mesh=mesh,
        in_specs=placed,
        out_specs=(P(("dp", "mp")), P(("dp", "mp"))),
        check_vma=False,
    )
```

```python
import functools

import jax
import jax.numpy as jnp
from jax import lax
from jax.experimental import pallas as pl
from jax.experimental.pallas import tpu as pltpu
from jax.sharding import PartitionSpec as P

ridge = 0.2
SUB = 8
MAX_ACC = 3
VALUE_MAX = 0.3
F32 = jnp.float32


def sublane_masks():
    sub = lax.broadcasted_iota(jnp.int32, (SUB, 128), 0)
    return [sub == s for s in range(SUB)]


def vmem_spec():
    return pl.BlockSpec(memory_space=pltpu.VMEM)


def smem_spec():
    return pl.BlockSpec(memory_space=pltpu.SMEM)


def any_spec():
    return pl.BlockSpec(memory_space=pl.ANY)


def hbm_spec():
    return pl.BlockSpec(memory_space=pltpu.HBM)


def entry(ref, base, offset):
    return ref.at[pl.ds(base + offset, 1)][0]


def params(megabytes):
    return pltpu.CompilerParams(vmem_limit_bytes=int(megabytes * 2**20))


def mib(*arrays):
    return sum(a.size * a.dtype.itemsize for a in arrays) / 2**20


def gram_body(hist, out):
    count, feats = hist.shape[1], hist.shape[2]
    width = 128

    def step(j, accs):
        at = pl.ds(pl.multiple_of(j * width, width), width)
        s_tile, y_tile = hist[0, :, at], hist[1, :, at]
        new = []
        for i in range(count):
            row = jnp.broadcast_to(y_tile[i : i + 1, :], (count, width))
            new.append((accs[i][0] + row * s_tile, accs[i][1] + row * y_tile))
        return tuple(new)

    zero = jnp.zeros((count, width), F32)
    accs = lax.fori_loop(0, feats // width, step, tuple((zero, zero) for _ in range(count)))
    lane = lax.broadcasted_iota(jnp.int32, (count, width), 1)
    for part in range(2):
        tile = zero
        for i in range(count):
            tile = jnp.where(lane == i, jnp.sum(accs[i][part], axis=1, keepdims=True), tile)
        out[part * count : (part + 1) * count, :] = tile


def chunk_copies(srcs, dsts, sems, c):
    n = sems.shape[1]
    copies = []
    for i, (src, dst) in enumerate(zip(srcs, dsts)):
        size = src.shape[0] // n
        at = pl.ds(c * size, size)
        copies.append(pltpu.make_async_copy(src.at[at], dst.at[at], sems.at[i, c]))
    return copies


def start_chunks(srcs, dsts, sems):
    for c in range(sems.shape[1]):
        for copy in chunk_copies(srcs, dsts, sems, c):
            copy.start()


def run_chunks(srcs, dsts, sems, trips, body):
    per = trips // sems.shape[1]

    def chunk(c, carry):
        for copy in chunk_copies(srcs, dsts, sems, c):
            copy.wait()
        return lax.fori_loop(c * per, (c + 1) * per, body, carry)

    lax.fori_loop(0, sems.shape[1], chunk, 0)


def fold_tiles(tiles):
    sub = lax.broadcasted_iota(jnp.int32, tiles[0].shape, 0)
    half = SUB // 2
    low = (sub & half) == 0
    tiles = [
        jnp.where(low, tiles[k], tiles[k + half]) + pltpu.roll(jnp.where(low, tiles[k + half], tiles[k]), half, 0)
        for k in range(half)
    ]
    while half > 1:
        half //= 2
        odd = (sub & half) != 0
        tiles = [
            jnp.where(
                odd,
                tiles[k + half] + pltpu.roll(tiles[k + half], half, 0),
                tiles[k] + pltpu.roll(tiles[k], SUB - half, 0),
            )
            for k in range(half)
        ]
    return tiles[0]


def gather_body(ids_in, vals_in, gram, *refs):
    *pieces, out, table, rows, vals, ids, sems = refs
    srcs, dsts = (ids_in, vals_in), (ids, vals)
    count, active, width = vals.shape
    start_chunks(srcs, dsts, sems)
    at = 0
    for piece in pieces:
        size = piece.shape[0]

        def widen(j, carry, piece=piece, at=at):
            src = pl.ds(pl.multiple_of(j * 64, 64), 64)
            dst = pl.ds(pl.multiple_of(j * 64 + at, 64), 64)
            table[dst, :] = piece[src, :].astype(F32)
            return carry

        lax.fori_loop(0, size // 64, widen, 0)
        at += size
    masks = sublane_masks()

    def group(g, carry):
        for u in range(SUB):
            e = g * SUB + u
            v = vals[e].astype(F32)
            total = None
            for t in range(0, active, SUB):
                pick = None
                for s in range(SUB):
                    row = table[pl.ds(entry(ids, e * active, t + s), SUB, stride=0), :]
                    pick = row if pick is None else jnp.where(masks[s], row, pick)
                prod = pick * v[t : t + SUB]
                total = prod if total is None else total + prod
            rows[pl.ds(e, 1), :] = jnp.sum(total, axis=0, keepdims=True)
        return carry

    run_chunks(srcs, dsts, sems, count // SUB, group)
    lines = count // width
    for b in range(lines):
        flipped = rows[b * width : (b + 1) * width, :].T
        out[b : b + 1, :] = jnp.sum(flipped, axis=0, keepdims=True)
    out[lines : lines + gram.shape[0], :] = gram[...]


def scatter_body(ids_in, resid, vals_in, *refs, order, owned):
    n_out = 2
    outs, accs = refs[:n_out], refs[n_out:-3]
    vals, ids, sems = refs[-3:]
    srcs, dsts = (ids_in, vals_in), (ids, vals)
    count, active, width = vals.shape
    start_chunks(srcs, dsts, sems)
    blocks = accs[0].shape[0] // SUB
    masks = sublane_masks()
    zero = jnp.zeros((SUB * SUB, width), F32)

    def clear(j, carry):
        at = pl.ds(pl.multiple_of(j * SUB * SUB, SUB * SUB), SUB * SUB)
        for acc in accs:
            acc[at, :] = zero
        return carry

    lax.fori_loop(0, blocks // SUB, clear, 0)
    unroll = 8

    def group(g, carry):
        turn = 0
        for u in range(unroll):
            e = g * unroll + u
            v = vals[e].astype(F32) * resid[e]
            for t in range(0, active, SUB):
                acc = accs[turn % len(accs)]
                turn += 1
                batch = []
                for s in range(SUB):
                    at = pl.ds(pl.multiple_of(entry(ids, e * active, t + s), SUB), SUB)
                    batch.append((at, acc[at, :] + v[t : t + SUB]))
                for s, (at, value) in enumerate(batch):
                    pltpu.store(acc.at[at, :], value, mask=masks[s])
        return carry

    run_chunks(srcs, dsts, sems, count // unroll, group)

    half = len(order) // 2
    for i, p in enumerate(order):
        out = outs[0] if i < half else outs[1]

        def fold(j, carry, p=p, out=out, base=(i % half) * owned):
            tiles = []
            for i in range(SUB):
                at = pl.ds(pl.multiple_of((p * owned + j * SUB + i) * SUB, SUB), SUB)
                total = accs[0][at, :]
                for acc in accs[1:]:
                    total = total + acc[at, :]
                tiles.append(total)
            out[pl.ds(pl.multiple_of(base + j * SUB, SUB), SUB), :] = fold_tiles(tiles)
            return carry

        lax.fori_loop(0, owned // SUB, fold, 0, unroll=2)


def dots_body(keep, recv, gram, w, hist, result, grad, dots):
    count, feats = hist.shape[1], hist.shape[2]
    rows, width = w.shape
    grad[...] = keep[...] + recv[...] + ridge * w[...]
    result[...] = grad[...]

    def step(j, accs):
        at = pl.ds(pl.multiple_of(j * width, width), width)
        g = grad[pl.ds(j, count, stride=0), :]
        return (accs[0] + g * hist[0, :, at], accs[1] + g * hist[1, :, at])

    zero = jnp.zeros((count, width), F32)
    accs = lax.fori_loop(0, feats // width, step, (zero, zero), unroll=8)
    dots[:count, :] = accs[0]
    dots[count : 2 * count, :] = accs[1]
    dots[2 * count :, :] = gram[...]


def coefficient_body(gram, out):
    count = gram.shape[0] // 2
    width = 128
    lane = lax.broadcasted_iota(jnp.int32, (1, width), 1)
    sy = lambda k, i: gram[k, i]
    yy = lambda k, i: gram[count + k, i]
    unit = lambda k: (lane == k).astype(F32)
    rho = [1.0 / jnp.full((1, width), sy(i, i), F32) for i in range(count)]
    last = count - 1
    gamma = jnp.full((1, width), sy(last, last), F32) / jnp.full((1, width), yy(last, last), F32)
    alpha = [None] * count
    for i in reversed(range(count)):
        value = unit(i)
        for j in range(i + 1, count):
            value = value - alpha[j] * sy(i, j)
        alpha[i] = rho[i] * value
    weight = []
    for i in range(count):
        value = unit(count + i)
        for j in range(count):
            value = value - alpha[j] * yy(i, j)
        value = gamma * value
        for k in range(i):
            value = value + weight[k] * sy(k, i)
        weight.append(alpha[i] - rho[i] * value)
    for k in range(count):
        out[k : k + 1, :] = weight[k]
        out[count + k : count + k + 1, :] = -gamma * alpha[k]
    out[2 * count :, :] = jnp.broadcast_to(gamma, (count, width))


def move_body(steps, coef, dots, recv, grad, w, hist, out):
    count = hist.shape[1]
    rows, width = w.shape
    sums = jnp.sum(dots[...] + recv[...], axis=1, keepdims=True)
    sub = lax.broadcasted_iota(jnp.int32, (2 * count, width), 0)
    lane = lax.broadcasted_iota(jnp.int32, (2 * count, width), 1)
    line = jnp.sum(jnp.where(sub == lane, sums, 0.0), axis=0, keepdims=True)
    mixed = jnp.sum(coef[: 2 * count, :] * line, axis=1, keepdims=True)
    c_s = jnp.broadcast_to(mixed[:count], (count, width))
    c_y = jnp.broadcast_to(mixed[count:], (count, width))
    gamma = coef[2 * count :, :]
    rate = steps[0]
    masks = sublane_masks()

    def step(j, carry):
        tile = jnp.zeros((SUB, width), F32)
        for u in range(SUB):
            at = pl.ds(pl.multiple_of((j * SUB + u) * width, width), width)
            mix = jnp.sum(c_s * hist[0, :, at] + c_y * hist[1, :, at], axis=0, keepdims=True)
            tile = jnp.where(masks[u], jnp.broadcast_to(mix, (SUB, width)), tile)
        at = pl.ds(pl.multiple_of(j * SUB, SUB), SUB)
        out[at, :] = w[at, :] - rate * (gamma * grad[at, :] + tile)
        return carry

    lax.fori_loop(0, rows // SUB, step, 0)


def gather_stages(n):
    stages = []
    top = n // 2
    while top >= 4:
        stages.append([top])
        top //= 2
    stages.append([k for k in (1, 2, 3) if k < n])
    return [s for s in stages if s]


def reduce_bits(n):
    bits = []
    b = 1
    while b < n:
        bits.append(b)
        b *= 2
    return bits


def xor_permute(x, axis, n, k):
    return lax.ppermute(x, axis, [(i, i ^ k) for i in range(n)])


def local(values, block_ids, labels, weights, history, steps, *, n_dp, n_mp):
    count, active, width = values.shape
    features = weights.shape[0]
    owned = features // width
    blocks = owned * n_dp
    pairs = history.shape[1]
    lines = count // width
    me = lax.axis_index("dp")
    w2 = weights.reshape(owned, width)
    values = pltpu.with_memory_space_constraint(values, pltpu.HBM)

    pieces = [w2.astype(jnp.bfloat16)]
    order = [0]
    for offsets in gather_stages(n_dp):
        whole = pieces[0] if len(pieces) == 1 else jnp.concatenate(pieces, axis=0)
        came = [xor_permute(whole, "dp", n_dp, k) for k in offsets]
        pieces = pieces + came
        order = order + [p ^ k for k in offsets for p in order]
    place = [0] * n_dp
    for at, p in enumerate(order):
        place[p] = at
    owner = block_ids // owned
    spot = owner ^ me
    where = jnp.zeros_like(spot)
    for p in range(n_dp):
        where = jnp.where(spot == p, place[p], where)
    flat_ids = (where * owned + (block_ids - owner * owned)).reshape(-1)

    gram = pl.pallas_call(
        gram_body,
        out_shape=jax.ShapeDtypeStruct((2 * pairs, width), F32),
        in_specs=[vmem_spec()],
        out_specs=vmem_spec(),
        compiler_params=params(2 * mib(history) + 2),
    )(history)

    streams = [
        pltpu.VMEM(values.shape, values.dtype),
        pltpu.SMEM((count * active,), jnp.int32),
        pltpu.SemaphoreType.DMA((2, 8)),
    ]
    table_mib = blocks * width * 4 / 2**20
    packed = pl.pallas_call(
        gather_body,
        out_shape=jax.ShapeDtypeStruct((lines + 2 * pairs, width), F32),
        in_specs=[any_spec(), hbm_spec(), vmem_spec()] + [vmem_spec()] * len(pieces),
        out_specs=vmem_spec(),
        scratch_shapes=[pltpu.VMEM((blocks, width), F32), pltpu.VMEM((count, width), F32)] + streams,
        compiler_params=params(mib(values) + 2 * table_mib + 6),
    )(flat_ids, values, gram, *pieces)

    packed = jnp.sum(lax.all_gather(packed, "mp", axis=0), axis=0)
    resid = jax.nn.sigmoid(packed[:lines].reshape(-1)) - labels.astype(F32)
    gram_rows = packed[lines:]

    bits = reduce_bits(n_dp)
    wanted = [0]
    for b in reversed(bits):
        wanted = [p ^ b for p in wanted] + wanted
    slots = [place[p] for p in wanted]

    acc_mib = SUB * table_mib
    room = (60 * 1024) / 1024 - mib(values) - table_mib - 6
    n_acc = max(1, min(MAX_ACC, int(room // acc_mib)))
    half = n_dp // 2 * owned
    send, keep = pl.pallas_call(
        functools.partial(scatter_body, order=slots, owned=owned),
        out_shape=[jax.ShapeDtypeStruct((half, width), F32)] * 2,
        in_specs=[any_spec(), smem_spec(), hbm_spec()],
        out_specs=[vmem_spec(), vmem_spec()],
        scratch_shapes=[pltpu.VMEM((blocks * SUB, width), F32)] * n_acc + streams,
        compiler_params=params(mib(values) + table_mib + n_acc * acc_mib + 3),
    )(flat_ids * SUB, resid, values)

    scale, bound = 1.0, VALUE_MAX * count * active * max(1, n_dp // 2)
    while bound * scale > 60000:
        scale /= 2
    for b in bits:
        sent = send if scale == 1.0 else send * scale
        came = xor_permute(sent.astype(jnp.float16), "dp", n_dp, b).astype(F32)
        came = came if scale == 1.0 else came / scale
        if b == bits[-1]:
            break
        total = keep + came
        cut = total.shape[0] // 2
        send, keep = total[:cut], total[cut:]

    result, grad, dots = pl.pallas_call(
        dots_body,
        out_shape=[
            jax.ShapeDtypeStruct((owned, width), F32),
            jax.ShapeDtypeStruct((owned, width), F32),
            jax.ShapeDtypeStruct((4 * pairs, width), F32),
        ],
        in_specs=[vmem_spec()] * 5,
        out_specs=[vmem_spec()] * 3,
        compiler_params=params(2 * mib(history) + 4),
    )(keep, came, gram_rows, w2, history)

    for b in bits:
        dots = dots + xor_permute(dots, "dp", n_dp, b)
    dots, gram_all = dots[: 2 * pairs], dots[2 * pairs :]

    coef = pl.pallas_call(
        coefficient_body,
        out_shape=jax.ShapeDtypeStruct((3 * pairs, width), F32),
        in_specs=[smem_spec()],
        out_specs=vmem_spec(),
        compiler_params=params(4),
    )(gram_all)

    hops = reduce_bits(n_mp)
    for b in hops[:-1]:
        dots = dots + xor_permute(dots, "mp", n_mp, b)
    other = xor_permute(dots, "mp", n_mp, hops[-1])

    moved = pl.pallas_call(
        move_body,
        out_shape=jax.ShapeDtypeStruct((owned, width), F32),
        in_specs=[smem_spec()] + [vmem_spec()] * 6,
        out_specs=vmem_spec(),
        compiler_params=params(2 * mib(history) + 4),
    )(steps, coef, dots, other, grad, w2, history)
    return moved.reshape(-1), result.reshape(-1)


def solution(mesh):
    placed = (
        P("dp", "mp", None),
        P("dp", "mp"),
        P("dp"),
        P(("dp", "mp")),
        P(None, None, ("dp", "mp")),
        P(),
    )
    return jax.shard_map(
        functools.partial(local, n_dp=mesh.shape["dp"], n_mp=mesh.shape["mp"]),
        mesh=mesh,
        in_specs=placed,
        out_specs=(P(("dp", "mp")), P(("dp", "mp"))),
        check_vma=False,
    )
```

```python
import functools

import jax
import jax.numpy as jnp
from jax import lax
from jax.experimental import pallas as pl
from jax.experimental.pallas import tpu as pltpu
from jax.sharding import PartitionSpec as P

ridge = 0.2
SUB = 8
MAX_ACC = 3
WIDE = 32
VALUE_MAX = 0.3
F32 = jnp.float32


def sublane_masks():
    sub = lax.broadcasted_iota(jnp.int32, (SUB, 128), 0)
    return [sub == s for s in range(SUB)]


def vmem_spec():
    return pl.BlockSpec(memory_space=pltpu.VMEM)


def smem_spec():
    return pl.BlockSpec(memory_space=pltpu.SMEM)


def any_spec():
    return pl.BlockSpec(memory_space=pl.ANY)


def hbm_spec():
    return pl.BlockSpec(memory_space=pltpu.HBM)


def entry(ref, base, offset):
    return ref.at[pl.ds(base + offset, 1)][0]


def params(megabytes):
    return pltpu.CompilerParams(vmem_limit_bytes=int(megabytes * 2**20))


def mib(*arrays):
    return sum(a.size * a.dtype.itemsize for a in arrays) / 2**20


def gram_body(hist, out):
    count, feats = hist.shape[1], hist.shape[2]
    width = 128

    def step(j, accs):
        at = pl.ds(pl.multiple_of(j * width, width), width)
        s_tile, y_tile = hist[0, :, at], hist[1, :, at]
        new = []
        for i in range(count):
            row = jnp.broadcast_to(y_tile[i : i + 1, :], (count, width))
            new.append((accs[i][0] + row * s_tile, accs[i][1] + row * y_tile))
        return tuple(new)

    zero = jnp.zeros((count, width), F32)
    accs = lax.fori_loop(0, feats // width, step, tuple((zero, zero) for _ in range(count)))
    lane = lax.broadcasted_iota(jnp.int32, (count, width), 1)
    for part in range(2):
        tile = zero
        for i in range(count):
            tile = jnp.where(lane == i, jnp.sum(accs[i][part], axis=1, keepdims=True), tile)
        out[part * count : (part + 1) * count, :] = tile


def chunk_copies(srcs, dsts, sems, c):
    n = sems.shape[1]
    copies = []
    for i, (src, dst) in enumerate(zip(srcs, dsts)):
        size = src.shape[0] // n
        at = pl.ds(c * size, size)
        copies.append(pltpu.make_async_copy(src.at[at], dst.at[at], sems.at[i, c]))
    return copies


def start_chunks(srcs, dsts, sems):
    for c in range(sems.shape[1]):
        for copy in chunk_copies(srcs, dsts, sems, c):
            copy.start()


def run_chunks(srcs, dsts, sems, trips, body):
    per = trips // sems.shape[1]

    def chunk(c, carry):
        for copy in chunk_copies(srcs, dsts, sems, c):
            copy.wait()
        return lax.fori_loop(c * per, (c + 1) * per, body, carry)

    lax.fori_loop(0, sems.shape[1], chunk, 0)


def fold_tiles(tiles):
    sub = lax.broadcasted_iota(jnp.int32, tiles[0].shape, 0)
    half = SUB // 2
    low = (sub & half) == 0
    tiles = [
        jnp.where(low, tiles[k], tiles[k + half]) + pltpu.roll(jnp.where(low, tiles[k + half], tiles[k]), half, 0)
        for k in range(half)
    ]
    while half > 1:
        half //= 2
        odd = (sub & half) != 0
        tiles = [
            jnp.where(
                odd,
                tiles[k + half] + pltpu.roll(tiles[k + half], half, 0),
                tiles[k] + pltpu.roll(tiles[k], SUB - half, 0),
            )
            for k in range(half)
        ]
    return tiles[0]


def gather_body(ids_in, vals_in, gram, *refs):
    *pieces, out, table, rows, vals, ids, sems = refs
    srcs, dsts = (ids_in, vals_in), (ids, vals)
    count, active, width = vals.shape
    start_chunks(srcs, dsts, sems)
    at = 0
    for piece in pieces:
        size = piece.shape[0]

        def widen(j, carry, piece=piece, at=at):
            src = pl.ds(pl.multiple_of(j * 64, 64), 64)
            dst = pl.ds(pl.multiple_of(j * 64 + at, 64), 64)
            table[dst, :] = piece[src, :].astype(F32)
            return carry

        lax.fori_loop(0, size // 64, widen, 0)
        at += size
    masks = sublane_masks()

    def group(g, carry):
        for u in range(WIDE):
            e = g * WIDE + u
            v = vals[e].astype(F32)
            total = None
            for t in range(0, active, SUB):
                pick = None
                for s in range(SUB):
                    row = table[pl.ds(entry(ids, e * active, t + s), SUB, stride=0), :]
                    pick = row if pick is None else jnp.where(masks[s], row, pick)
                prod = pick * v[t : t + SUB]
                total = prod if total is None else total + prod
            rows[pl.ds(e, 1), :] = jnp.sum(total, axis=0, keepdims=True)
        return carry

    run_chunks(srcs, dsts, sems, count // WIDE, group)
    lines = count // width
    for b in range(lines):
        flipped = rows[b * width : (b + 1) * width, :].T
        out[b : b + 1, :] = jnp.sum(flipped, axis=0, keepdims=True)
    out[lines : lines + gram.shape[0], :] = gram[...]


def scatter_body(ids_in, resid_in, vals_in, *refs, order, owned):
    n_out = 2
    outs, accs = refs[:n_out], refs[n_out:-5]
    resid, resid_sem, vals, ids, sems = refs[-5:]
    resid_copy = pltpu.make_async_copy(resid_in, resid, resid_sem)
    resid_copy.start()
    srcs, dsts = (ids_in, vals_in), (ids, vals)
    count, active, width = vals.shape
    start_chunks(srcs, dsts, sems)
    blocks = accs[0].shape[0] // SUB
    masks = sublane_masks()
    zero = jnp.zeros((SUB * SUB, width), F32)

    def clear(j, carry):
        at = pl.ds(pl.multiple_of(j * SUB * SUB, SUB * SUB), SUB * SUB)
        for acc in accs:
            acc[at, :] = zero
        return carry

    lax.fori_loop(0, blocks // SUB, clear, 0)
    resid_copy.wait()
    unroll = WIDE

    def group(g, carry):
        turn = 0
        for u in range(unroll):
            e = g * unroll + u
            v = vals[e].astype(F32) * resid[e]
            for t in range(0, active, SUB):
                acc = accs[turn % len(accs)]
                turn += 1
                batch = []
                for s in range(SUB):
                    at = pl.ds(pl.multiple_of(entry(ids, e * active, t + s), SUB), SUB)
                    batch.append((at, acc[at, :] + v[t : t + SUB]))
                for s, (at, value) in enumerate(batch):
                    pltpu.store(acc.at[at, :], value, mask=masks[s])
        return carry

    run_chunks(srcs, dsts, sems, count // unroll, group)

    half = len(order) // 2
    for i, p in enumerate(order):
        out = outs[0] if i < half else outs[1]

        def fold(j, carry, p=p, out=out, base=(i % half) * owned):
            tiles = []
            for i in range(SUB):
                at = pl.ds(pl.multiple_of((p * owned + j * SUB + i) * SUB, SUB), SUB)
                total = accs[0][at, :]
                for acc in accs[1:]:
                    total = total + acc[at, :]
                tiles.append(total)
            out[pl.ds(pl.multiple_of(base + j * SUB, SUB), SUB), :] = fold_tiles(tiles)
            return carry

        lax.fori_loop(0, owned // SUB, fold, 0, unroll=4)


def dots_body(keep, recv, gram, w, hist, result, grad, dots):
    count, feats = hist.shape[1], hist.shape[2]
    rows, width = w.shape
    grad[...] = keep[...] + recv[...] + ridge * w[...]
    result[...] = grad[...]

    def step(j, accs):
        at = pl.ds(pl.multiple_of(j * width, width), width)
        g = grad[pl.ds(j, count, stride=0), :]
        return (accs[0] + g * hist[0, :, at], accs[1] + g * hist[1, :, at])

    zero = jnp.zeros((count, width), F32)
    accs = lax.fori_loop(0, feats // width, step, (zero, zero), unroll=8)
    dots[:count, :] = accs[0]
    dots[count : 2 * count, :] = accs[1]
    dots[2 * count :, :] = gram[...]


def coefficient_body(gram, out):
    count = gram.shape[0] // 2
    width = 128
    lane = lax.broadcasted_iota(jnp.int32, (1, width), 1)
    sy = lambda k, i: gram[k, i]
    yy = lambda k, i: gram[count + k, i]
    unit = lambda k: (lane == k).astype(F32)
    rho = [1.0 / jnp.full((1, width), sy(i, i), F32) for i in range(count)]
    last = count - 1
    gamma = jnp.full((1, width), sy(last, last), F32) / jnp.full((1, width), yy(last, last), F32)
    alpha = [None] * count
    for i in reversed(range(count)):
        value = unit(i)
        for j in range(i + 1, count):
            value = value - alpha[j] * sy(i, j)
        alpha[i] = rho[i] * value
    weight = []
    for i in range(count):
        value = unit(count + i)
        for j in range(count):
            value = value - alpha[j] * yy(i, j)
        value = gamma * value
        for k in range(i):
            value = value + weight[k] * sy(k, i)
        weight.append(alpha[i] - rho[i] * value)
    for k in range(count):
        out[k : k + 1, :] = weight[k]
        out[count + k : count + k + 1, :] = -gamma * alpha[k]
    out[2 * count :, :] = jnp.broadcast_to(gamma, (count, width))


def move_body(steps, coef, dots, recv, grad, w, hist, out):
    count = hist.shape[1]
    rows, width = w.shape
    sums = jnp.sum(dots[...] + recv[...], axis=1, keepdims=True)
    sub = lax.broadcasted_iota(jnp.int32, (2 * count, width), 0)
    lane = lax.broadcasted_iota(jnp.int32, (2 * count, width), 1)
    line = jnp.sum(jnp.where(sub == lane, sums, 0.0), axis=0, keepdims=True)
    mixed = jnp.sum(coef[: 2 * count, :] * line, axis=1, keepdims=True)
    c_s = jnp.broadcast_to(mixed[:count], (count, width))
    c_y = jnp.broadcast_to(mixed[count:], (count, width))
    gamma = coef[2 * count :, :]
    rate = steps[0]

    def step(j, carry):
        tiles = []
        for u in range(SUB):
            at = pl.ds(pl.multiple_of((j * SUB + u) * width, width), width)
            tiles.append(c_s * hist[0, :, at] + c_y * hist[1, :, at])
        tile = fold_tiles(tiles)
        at = pl.ds(pl.multiple_of(j * SUB, SUB), SUB)
        out[at, :] = w[at, :] - rate * (gamma * grad[at, :] + tile)
        return carry

    lax.fori_loop(0, rows // SUB, step, 0, unroll=2)


def gather_stages(n):
    stages = []
    top = n // 2
    while top >= 4:
        stages.append([top])
        top //= 2
    stages.append([k for k in (1, 2, 3) if k < n])
    return [s for s in stages if s]


def reduce_bits(n):
    bits = []
    b = 1
    while b < n:
        bits.append(b)
        b *= 2
    return bits


def xor_permute(x, axis, n, k):
    return lax.ppermute(x, axis, [(i, i ^ k) for i in range(n)])


def local(values, block_ids, labels, weights, history, steps, *, n_dp, n_mp):
    count, active, width = values.shape
    features = weights.shape[0]
    owned = features // width
    blocks = owned * n_dp
    pairs = history.shape[1]
    lines = count // width
    me = lax.axis_index("dp")
    w2 = weights.reshape(owned, width)
    values = pltpu.with_memory_space_constraint(values, pltpu.HBM)

    pieces = [w2.astype(jnp.bfloat16)]
    order = [0]
    for offsets in gather_stages(n_dp):
        whole = pieces[0] if len(pieces) == 1 else jnp.concatenate(pieces, axis=0)
        whole, late_history = lax.optimization_barrier((whole, history))
        came = [xor_permute(whole, "dp", n_dp, k) for k in offsets]
        pieces = pieces + came
        order = order + [p ^ k for k in offsets for p in order]
    place = [0] * n_dp
    for at, p in enumerate(order):
        place[p] = at
    owner = block_ids // owned
    spot = owner ^ me
    where = jnp.zeros_like(spot)
    for p in range(n_dp):
        where = jnp.where(spot == p, place[p], where)
    flat_ids = (where * owned + (block_ids - owner * owned)).reshape(-1)

    gram = pl.pallas_call(
        gram_body,
        out_shape=jax.ShapeDtypeStruct((2 * pairs, width), F32),
        in_specs=[vmem_spec()],
        out_specs=vmem_spec(),
        compiler_params=params(2 * mib(history) + 2),
    )(late_history)

    streams = [
        pltpu.VMEM(values.shape, values.dtype),
        pltpu.SMEM((count * active,), jnp.int32),
        pltpu.SemaphoreType.DMA((2, 8)),
    ]
    table_mib = blocks * width * 4 / 2**20
    packed = pl.pallas_call(
        gather_body,
        out_shape=jax.ShapeDtypeStruct((lines + 2 * pairs, width), F32),
        in_specs=[any_spec(), hbm_spec(), vmem_spec()] + [vmem_spec()] * len(pieces),
        out_specs=vmem_spec(),
        scratch_shapes=[pltpu.VMEM((blocks, width), F32), pltpu.VMEM((count, width), F32)] + streams,
        compiler_params=params(mib(values) + 2 * table_mib + 6),
    )(flat_ids, values, gram, *pieces)

    for b in reduce_bits(n_mp):
        packed = packed + xor_permute(packed, "mp", n_mp, b)
    resid = jax.nn.sigmoid(packed[:lines].reshape(-1)) - labels.astype(F32)
    gram_rows = packed[lines:]

    bits = reduce_bits(n_dp)
    wanted = [0]
    for b in reversed(bits):
        wanted = [p ^ b for p in wanted] + wanted
    slots = [place[p] for p in wanted]

    acc_mib = SUB * table_mib
    room = (60 * 1024) / 1024 - mib(values) - table_mib - 6
    n_acc = max(1, min(MAX_ACC, int(room // acc_mib)))
    half = n_dp // 2 * owned
    send, keep = pl.pallas_call(
        functools.partial(scatter_body, order=slots, owned=owned),
        out_shape=[jax.ShapeDtypeStruct((half, width), F32)] * 2,
        in_specs=[any_spec(), any_spec(), hbm_spec()],
        out_specs=[vmem_spec(), vmem_spec()],
        scratch_shapes=[pltpu.VMEM((blocks * SUB, width), F32)] * n_acc
        + [pltpu.SMEM((count,), F32), pltpu.SemaphoreType.DMA]
        + streams,
        compiler_params=params(mib(values) + table_mib + n_acc * acc_mib + 3),
    )(flat_ids * SUB, resid, values)

    scale, bound = 1.0, VALUE_MAX * count * active * max(1, n_dp // 2)
    while bound * scale > 60000:
        scale /= 2
    for b in bits:
        sent = send if scale == 1.0 else send * scale
        came = xor_permute(sent.astype(jnp.float16), "dp", n_dp, b).astype(F32)
        came = came if scale == 1.0 else came / scale
        if b == bits[-1]:
            break
        total = keep + came
        cut = total.shape[0] // 2
        send, keep = total[:cut], total[cut:]

    result, grad, dots = pl.pallas_call(
        dots_body,
        out_shape=[
            jax.ShapeDtypeStruct((owned, width), F32),
            jax.ShapeDtypeStruct((owned, width), F32),
            jax.ShapeDtypeStruct((4 * pairs, width), F32),
        ],
        in_specs=[vmem_spec()] * 5,
        out_specs=[vmem_spec()] * 3,
        compiler_params=params(2 * mib(history) + 4),
    )(keep, came, gram_rows, w2, history)

    for b in bits:
        dots = dots + xor_permute(dots, "dp", n_dp, b)
    dots, gram_all = dots[: 2 * pairs], dots[2 * pairs :]

    coef = pl.pallas_call(
        coefficient_body,
        out_shape=jax.ShapeDtypeStruct((3 * pairs, width), F32),
        in_specs=[smem_spec()],
        out_specs=vmem_spec(),
        compiler_params=params(4),
    )(gram_all)

    hops = reduce_bits(n_mp)
    for b in hops[:-1]:
        dots = dots + xor_permute(dots, "mp", n_mp, b)
    other = xor_permute(dots, "mp", n_mp, hops[-1])

    moved = pl.pallas_call(
        move_body,
        out_shape=jax.ShapeDtypeStruct((owned, width), F32),
        in_specs=[smem_spec()] + [vmem_spec()] * 6,
        out_specs=vmem_spec(),
        compiler_params=params(2 * mib(history) + 4),
    )(steps, coef, dots, other, grad, w2, history)
    return moved.reshape(-1), result.reshape(-1)


def solution(mesh):
    placed = (
        P("dp", "mp", None),
        P("dp", "mp"),
        P("dp"),
        P(("dp", "mp")),
        P(None, None, ("dp", "mp")),
        P(),
    )
    return jax.shard_map(
        functools.partial(local, n_dp=mesh.shape["dp"], n_mp=mesh.shape["mp"]),
        mesh=mesh,
        in_specs=placed,
        out_specs=(P(("dp", "mp")), P(("dp", "mp"))),
        check_vma=False,
    )
```

```python
import functools

import jax
import jax.numpy as jnp
from jax import lax
from jax.experimental import pallas as pl
from jax.experimental.pallas import tpu as pltpu
from jax.sharding import PartitionSpec as P

ridge = 0.2
SUB = 8
MAX_ACC = 3
WIDE = 32
VALUE_MAX = 0.3
F32 = jnp.float32


def sublane_masks():
    sub = lax.broadcasted_iota(jnp.int32, (SUB, 128), 0)
    return [sub == s for s in range(SUB)]


def vmem_spec():
    return pl.BlockSpec(memory_space=pltpu.VMEM)


def smem_spec():
    return pl.BlockSpec(memory_space=pltpu.SMEM)


def any_spec():
    return pl.BlockSpec(memory_space=pl.ANY)


def hbm_spec():
    return pl.BlockSpec(memory_space=pltpu.HBM)


def entry(ref, base, offset):
    return ref.at[pl.ds(base + offset, 1)][0]


def params(megabytes):
    return pltpu.CompilerParams(vmem_limit_bytes=int(megabytes * 2**20))


def mib(*arrays):
    return sum(a.size * a.dtype.itemsize for a in arrays) / 2**20


def gram_body(hist, out):
    count, feats = hist.shape[1], hist.shape[2]
    width = 128

    def step(j, accs):
        at = pl.ds(pl.multiple_of(j * width, width), width)
        s_tile, y_tile = hist[0, :, at], hist[1, :, at]
        new = []
        for i in range(count):
            row = jnp.broadcast_to(y_tile[i : i + 1, :], (count, width))
            new.append((accs[i][0] + row * s_tile, accs[i][1] + row * y_tile))
        return tuple(new)

    zero = jnp.zeros((count, width), F32)
    accs = lax.fori_loop(0, feats // width, step, tuple((zero, zero) for _ in range(count)))
    lane = lax.broadcasted_iota(jnp.int32, (count, width), 1)
    for part in range(2):
        tile = zero
        for i in range(count):
            tile = jnp.where(lane == i, jnp.sum(accs[i][part], axis=1, keepdims=True), tile)
        out[part * count : (part + 1) * count, :] = tile


def chunk_copies(srcs, dsts, sems, c):
    n = sems.shape[1]
    copies = []
    for i, (src, dst) in enumerate(zip(srcs, dsts)):
        size = src.shape[0] // n
        at = pl.ds(c * size, size)
        copies.append(pltpu.make_async_copy(src.at[at], dst.at[at], sems.at[i, c]))
    return copies


def start_chunks(srcs, dsts, sems):
    for c in range(sems.shape[1]):
        for copy in chunk_copies(srcs, dsts, sems, c):
            copy.start()


def run_chunks(srcs, dsts, sems, trips, body):
    per = trips // sems.shape[1]

    def chunk(c, carry):
        for copy in chunk_copies(srcs, dsts, sems, c):
            copy.wait()
        return lax.fori_loop(c * per, (c + 1) * per, body, carry)

    lax.fori_loop(0, sems.shape[1], chunk, 0)


def fold_tiles(tiles):
    sub = lax.broadcasted_iota(jnp.int32, tiles[0].shape, 0)
    half = SUB // 2
    low = (sub & half) == 0
    tiles = [
        jnp.where(low, tiles[k], tiles[k + half]) + pltpu.roll(jnp.where(low, tiles[k + half], tiles[k]), half, 0)
        for k in range(half)
    ]
    while half > 1:
        half //= 2
        odd = (sub & half) != 0
        tiles = [
            jnp.where(
                odd,
                tiles[k + half] + pltpu.roll(tiles[k + half], half, 0),
                tiles[k] + pltpu.roll(tiles[k], SUB - half, 0),
            )
            for k in range(half)
        ]
    return tiles[0]


def gather_body(ids_in, vals_in, gram, *refs):
    *pieces, out, table, rows, vals, ids, sems = refs
    srcs, dsts = (ids_in, vals_in), (ids, vals)
    count, active, width = vals.shape
    start_chunks(srcs, dsts, sems)
    at = 0
    for piece in pieces:
        size = piece.shape[0]

        def widen(j, carry, piece=piece, at=at):
            src = pl.ds(pl.multiple_of(j * 64, 64), 64)
            dst = pl.ds(pl.multiple_of(j * 64 + at, 64), 64)
            table[dst, :] = piece[src, :].astype(F32)
            return carry

        lax.fori_loop(0, size // 64, widen, 0)
        at += size
    masks = sublane_masks()

    def group(g, carry):
        for u in range(WIDE):
            e = g * WIDE + u
            v = vals[e].astype(F32)
            total = None
            for t in range(0, active, SUB):
                pick = None
                for s in range(SUB):
                    row = table[pl.ds(entry(ids, e * active, t + s), SUB, stride=0), :]
                    pick = row if pick is None else jnp.where(masks[s], row, pick)
                prod = pick * v[t : t + SUB]
                total = prod if total is None else total + prod
            rows[pl.ds(e, 1), :] = jnp.sum(total, axis=0, keepdims=True)
        return carry

    run_chunks(srcs, dsts, sems, count // WIDE, group)
    lines = count // width
    for b in range(lines):
        flipped = rows[b * width : (b + 1) * width, :].T
        out[b : b + 1, :] = jnp.sum(flipped, axis=0, keepdims=True)
    out[lines : lines + gram.shape[0], :] = gram[...]


def scatter_body(ids_in, resid_in, vals_in, *refs, orders, owned):
    n_out = len(orders)
    outs, accs = refs[:n_out], refs[n_out:-5]
    resid, resid_sem, vals, ids, sems = refs[-5:]
    resid_copy = pltpu.make_async_copy(resid_in, resid, resid_sem)
    resid_copy.start()
    srcs, dsts = (ids_in, vals_in), (ids, vals)
    count, active, width = vals.shape
    start_chunks(srcs, dsts, sems)
    blocks = accs[0].shape[0] // SUB
    masks = sublane_masks()
    zero = jnp.zeros((SUB * SUB, width), F32)

    def clear(j, carry):
        at = pl.ds(pl.multiple_of(j * SUB * SUB, SUB * SUB), SUB * SUB)
        for acc in accs:
            acc[at, :] = zero
        return carry

    lax.fori_loop(0, blocks // SUB, clear, 0)
    resid_copy.wait()
    unroll = WIDE

    def group(g, carry):
        turn = 0
        for u in range(unroll):
            e = g * unroll + u
            v = vals[e].astype(F32) * resid[e]
            for t in range(0, active, SUB):
                acc = accs[turn % len(accs)]
                turn += 1
                batch = []
                for s in range(SUB):
                    at = pl.ds(pl.multiple_of(entry(ids, e * active, t + s), SUB), SUB)
                    batch.append((at, acc[at, :] + v[t : t + SUB]))
                for s, (at, value) in enumerate(batch):
                    pltpu.store(acc.at[at, :], value, mask=masks[s])
        return carry

    run_chunks(srcs, dsts, sems, count // unroll, group)

    for i, p, out in [(i, p, out) for order, out in zip(orders, outs) for i, p in enumerate(order)]:

        def fold(j, carry, p=p, out=out, base=i * owned):
            tiles = []
            for i in range(SUB):
                at = pl.ds(pl.multiple_of((p * owned + j * SUB + i) * SUB, SUB), SUB)
                total = accs[0][at, :]
                for acc in accs[1:]:
                    total = total + acc[at, :]
                tiles.append(total)
            out[pl.ds(pl.multiple_of(base + j * SUB, SUB), SUB), :] = fold_tiles(tiles)
            return carry

        lax.fori_loop(0, owned // SUB, fold, 0, unroll=4)


def dots_body(keep, recv, gram, w, hist, result, grad, dots):
    count, feats = hist.shape[1], hist.shape[2]
    rows, width = w.shape
    grad[...] = keep[...] + recv[...] + ridge * w[...]
    result[...] = grad[...]

    def step(j, accs):
        at = pl.ds(pl.multiple_of(j * width, width), width)
        g = grad[pl.ds(j, count, stride=0), :]
        return (accs[0] + g * hist[0, :, at], accs[1] + g * hist[1, :, at])

    zero = jnp.zeros((count, width), F32)
    accs = lax.fori_loop(0, feats // width, step, (zero, zero), unroll=8)
    dots[:count, :] = accs[0]
    dots[count : 2 * count, :] = accs[1]
    dots[2 * count :, :] = gram[...]


def coefficient_body(gram, out):
    count = gram.shape[0] // 2
    width = 128
    lane = lax.broadcasted_iota(jnp.int32, (1, width), 1)
    sy = lambda k, i: gram[k, i]
    yy = lambda k, i: gram[count + k, i]
    unit = lambda k: (lane == k).astype(F32)
    rho = [1.0 / jnp.full((1, width), sy(i, i), F32) for i in range(count)]
    last = count - 1
    gamma = jnp.full((1, width), sy(last, last), F32) / jnp.full((1, width), yy(last, last), F32)
    alpha = [None] * count
    for i in reversed(range(count)):
        value = unit(i)
        for j in range(i + 1, count):
            value = value - alpha[j] * sy(i, j)
        alpha[i] = rho[i] * value
    weight = []
    for i in range(count):
        value = unit(count + i)
        for j in range(count):
            value = value - alpha[j] * yy(i, j)
        value = gamma * value
        for k in range(i):
            value = value + weight[k] * sy(k, i)
        weight.append(alpha[i] - rho[i] * value)
    for k in range(count):
        out[k : k + 1, :] = weight[k]
        out[count + k : count + k + 1, :] = -gamma * alpha[k]
    out[2 * count :, :] = jnp.broadcast_to(gamma, (count, width))


def move_body(steps, coef, dots, recv, grad, w, hist, out):
    count = hist.shape[1]
    rows, width = w.shape
    sums = jnp.sum(dots[...] + recv[...], axis=1, keepdims=True)
    sub = lax.broadcasted_iota(jnp.int32, (2 * count, width), 0)
    lane = lax.broadcasted_iota(jnp.int32, (2 * count, width), 1)
    line = jnp.sum(jnp.where(sub == lane, sums, 0.0), axis=0, keepdims=True)
    mixed = jnp.sum(coef[: 2 * count, :] * line, axis=1, keepdims=True)
    c_s = jnp.broadcast_to(mixed[:count], (count, width))
    c_y = jnp.broadcast_to(mixed[count:], (count, width))
    gamma = coef[2 * count :, :]
    rate = steps[0]

    def step(j, carry):
        tiles = []
        for u in range(SUB):
            at = pl.ds(pl.multiple_of((j * SUB + u) * width, width), width)
            tiles.append(c_s * hist[0, :, at] + c_y * hist[1, :, at])
        tile = fold_tiles(tiles)
        at = pl.ds(pl.multiple_of(j * SUB, SUB), SUB)
        out[at, :] = w[at, :] - rate * (gamma * grad[at, :] + tile)
        return carry

    lax.fori_loop(0, rows // SUB, step, 0, unroll=2)


def gather_stages(n):
    stages = []
    top = n // 2
    while top >= 4:
        stages.append([top])
        top //= 2
    stages.append([k for k in (1, 2, 3) if k < n])
    return [s for s in stages if s]


def reduce_bits(n):
    bits = []
    b = 1
    while b < n:
        bits.append(b)
        b *= 2
    return bits


def xor_permute(x, axis, n, k):
    return lax.ppermute(x, axis, [(i, i ^ k) for i in range(n)])


def local(values, block_ids, labels, weights, history, steps, *, n_dp, n_mp):
    count, active, width = values.shape
    features = weights.shape[0]
    owned = features // width
    blocks = owned * n_dp
    pairs = history.shape[1]
    lines = count // width
    me = lax.axis_index("dp")
    w2 = weights.reshape(owned, width)
    values = pltpu.with_memory_space_constraint(values, pltpu.HBM)

    pieces = [w2.astype(jnp.bfloat16)]
    order = [0]
    for offsets in gather_stages(n_dp):
        whole = pieces[0] if len(pieces) == 1 else jnp.concatenate(pieces, axis=0)
        whole, late_history = lax.optimization_barrier((whole, history))
        came = [xor_permute(whole, "dp", n_dp, k) for k in offsets]
        pieces = pieces + came
        order = order + [p ^ k for k in offsets for p in order]
    place = [0] * n_dp
    for at, p in enumerate(order):
        place[p] = at
    owner = block_ids // owned
    spot = owner ^ me
    where = jnp.zeros_like(spot)
    for p in range(n_dp):
        where = jnp.where(spot == p, place[p], where)
    flat_ids = (where * owned + (block_ids - owner * owned)).reshape(-1)

    gram = pl.pallas_call(
        gram_body,
        out_shape=jax.ShapeDtypeStruct((2 * pairs, width), F32),
        in_specs=[vmem_spec()],
        out_specs=vmem_spec(),
        compiler_params=params(2 * mib(history) + 2),
    )(late_history)

    streams = [
        pltpu.VMEM(values.shape, values.dtype),
        pltpu.SMEM((count * active,), jnp.int32),
        pltpu.SemaphoreType.DMA((2, 8)),
    ]
    table_mib = blocks * width * 4 / 2**20
    packed = pl.pallas_call(
        gather_body,
        out_shape=jax.ShapeDtypeStruct((lines + 2 * pairs, width), F32),
        in_specs=[any_spec(), hbm_spec(), vmem_spec()] + [vmem_spec()] * len(pieces),
        out_specs=vmem_spec(),
        scratch_shapes=[pltpu.VMEM((blocks, width), F32), pltpu.VMEM((count, width), F32)] + streams,
        compiler_params=params(mib(values) + 2 * table_mib + 6),
    )(flat_ids, values, gram, *pieces)

    for b in reduce_bits(n_mp):
        packed = packed + xor_permute(packed, "mp", n_mp, b)
    resid = jax.nn.sigmoid(packed[:lines].reshape(-1)) - labels.astype(F32)
    gram_rows = packed[lines:]

    bits = reduce_bits(n_dp)
    direct = [k for k in (1, 2, 3) if k < n_dp]
    wanted = [0]
    for b in reversed(bits[2:]):
        wanted = [p ^ b for p in wanted] + wanted
    slots = [[place[p ^ k] for p in wanted] for k in direct + [0]]

    acc_mib = SUB * table_mib
    room = (60 * 1024) / 1024 - mib(values) - table_mib - 6
    n_acc = max(1, min(MAX_ACC, int(room // acc_mib)))
    part = len(wanted) * owned
    *sends, keep = pl.pallas_call(
        functools.partial(scatter_body, orders=slots, owned=owned),
        out_shape=[jax.ShapeDtypeStruct((part, width), F32)] * len(slots),
        in_specs=[any_spec(), any_spec(), hbm_spec()],
        out_specs=[vmem_spec()] * len(slots),
        scratch_shapes=[pltpu.VMEM((blocks * SUB, width), F32)] * n_acc
        + [pltpu.SMEM((count,), F32), pltpu.SemaphoreType.DMA]
        + streams,
        compiler_params=params(mib(values) + table_mib + n_acc * acc_mib + 3),
    )(flat_ids * SUB, resid, values)

    scale, bound = 1.0, VALUE_MAX * count * active * max(1, n_dp // 2)
    while bound * scale > 60000:
        scale /= 2

    def partner(x, k):
        sent = x if scale == 1.0 else x * scale
        came = xor_permute(sent.astype(jnp.float16), "dp", n_dp, k).astype(F32)
        return came if scale == 1.0 else came / scale

    came = [partner(send, k) for send, k in zip(sends, direct)]
    for b in bits[2:]:
        total = functools.reduce(jnp.add, came, keep)
        cut = total.shape[0] // 2
        came = [partner(total[:cut], b)]
        keep = total[cut:]
    came = functools.reduce(jnp.add, came)

    result, grad, dots = pl.pallas_call(
        dots_body,
        out_shape=[
            jax.ShapeDtypeStruct((owned, width), F32),
            jax.ShapeDtypeStruct((owned, width), F32),
            jax.ShapeDtypeStruct((4 * pairs, width), F32),
        ],
        in_specs=[vmem_spec()] * 5,
        out_specs=[vmem_spec()] * 3,
        compiler_params=params(2 * mib(history) + 4),
    )(keep, came, gram_rows, w2, history)

    for b in bits:
        dots = dots + xor_permute(dots, "dp", n_dp, b)
    dots, gram_all = dots[: 2 * pairs], dots[2 * pairs :]

    coef = pl.pallas_call(
        coefficient_body,
        out_shape=jax.ShapeDtypeStruct((3 * pairs, width), F32),
        in_specs=[smem_spec()],
        out_specs=vmem_spec(),
        compiler_params=params(4),
    )(gram_all)

    hops = reduce_bits(n_mp)
    for b in hops[:-1]:
        dots = dots + xor_permute(dots, "mp", n_mp, b)
    other = xor_permute(dots, "mp", n_mp, hops[-1])

    moved = pl.pallas_call(
        move_body,
        out_shape=jax.ShapeDtypeStruct((owned, width), F32),
        in_specs=[smem_spec()] + [vmem_spec()] * 6,
        out_specs=vmem_spec(),
        compiler_params=params(2 * mib(history) + 4),
    )(steps, coef, dots, other, grad, w2, history)
    return moved.reshape(-1), result.reshape(-1)


def solution(mesh):
    placed = (
        P("dp", "mp", None),
        P("dp", "mp"),
        P("dp"),
        P(("dp", "mp")),
        P(None, None, ("dp", "mp")),
        P(),
    )
    return jax.shard_map(
        functools.partial(local, n_dp=mesh.shape["dp"], n_mp=mesh.shape["mp"]),
        mesh=mesh,
        in_specs=placed,
        out_specs=(P(("dp", "mp")), P(("dp", "mp"))),
        check_vma=False,
    )
```
